8 devices in a mesh: cp: 8 (over z, y, x, core).
Axes of the slice: x: 2, y: 2, z: 1, core: 2. Of those that a mesh axis runs over, the one named last changes fastest.
Arguments:
- act_in: bfloat16 [1, 4096, 1536], P(None, 'cp')
- grad_out: bfloat16 [1, 4096, 1536], P(None, 'cp')
- l1_norm1_gain: bfloat16 [1536], replicated
- l1_norm1_bias: bfloat16 [1536], replicated
- l1_qkv_w: bfloat16 [1536, 3, 16, 96], replicated
- l1_qkv_b: bfloat16 [3, 16, 96], replicated
- l1_out_w: bfloat16 [16, 96, 1536], replicated
- l1_out_b: bfloat16 [1536], replicated
- l1_norm2_gain: bfloat16 [1536], replicated
- l1_norm2_bias: bfloat16 [1536], replicated
- l1_up_w: bfloat16 [1536, 6144], replicated
- l1_up_b: bfloat16 [6144], replicated
- l1_down_w: bfloat16 [6144, 1536], replicated
- l1_down_b: bfloat16 [1536], replicated
- l2_norm1_gain: bfloat16 [1536], replicated
- l2_norm1_bias: bfloat16 [1536], replicated
- l2_qkv_w: bfloat16 [1536, 3, 16, 96], replicated
- l2_qkv_b: bfloat16 [3, 16, 96], replicated
- l2_out_w: bfloat16 [16, 96, 1536], replicated
- l2_out_b: bfloat16 [1536], replicated
- l2_norm2_gain: bfloat16 [1536], replicated
- l2_norm2_bias: bfloat16 [1536], replicated
- l2_up_w: bfloat16 [1536, 6144], replicated
- l2_up_b: bfloat16 [6144], replicated
- l2_down_w: bfloat16 [6144, 1536], replicated
- l2_down_b: bfloat16 [1536], replicated
Outputs:
- output 1: bfloat16 [1, 4096, 1536], P(None, 'cp')
- output 2: bfloat16 [1, 4096, 1536], P(None, 'cp')
- output 3: float32 [1536], replicated
- output 4: float32 [1536], replicated
- output 5: float32 [1536, 3, 16, 96], replicated
- output 6: float32 [3, 16, 96], replicated
- output 7: float32 [16, 96, 1536], replicated
- output 8: float32 [1536], replicated
- output 9: float32 [1536], replicated
- output 10: float32 [1536], replicated
- output 11: float32 [1536, 6144], replicated
- output 12: float32 [6144], replicated
- output 13: float32 [6144, 1536], replicated
- output 14: float32 [1536], replicated
- output 15: float32 [1536], replicated
- output 16: float32 [1536], replicated
- output 17: float32 [1536, 3, 16, 96], replicated
- output 18: float32 [3, 16, 96], replicated
- output 19: float32 [16, 96, 1536], replicated
- output 20: float32 [1536], replicated
- output 21: float32 [1536], replicated
- output 22: float32 [1536], replicated
- output 23: float32 [1536, 6144], replicated
- output 24: float32 [6144], replicated
- output 25: float32 [6144, 1536], replicated
- output 26: float32 [1536], replicated
All inputs are finite; a program needn't handle non-finite values.
Results may differ from the reference program's by a relative error of at most 0.0180966.
Values are sent between devices in bfloat16 or wider.
A program may use at most 1.5 GiB of HBM per device.

```python
import jax
import jax.numpy as jnp
from jax import lax

BATCH = 1
SEQ_DEV = 512
BLOCKS = 8
D = 1536
HEADS = 16
HEAD = 96
WINDOW = 256
SEQ = BLOCKS * SEQ_DEV
FF = 4 * D
HIDDEN = HEADS * HEAD


def draw_layer(key_list, prefix):
    def gaussian(draw_id, arr_shape):
        return jax.random.normal(key_list[draw_id], arr_shape, jnp.float32)
    return {
        prefix + "norm1_gain": (1.0 + 0.2 * gaussian(0, (D,))).astype(jnp.bfloat16),
        prefix + "norm1_bias": (0.2 * gaussian(1, (D,))).astype(jnp.bfloat16),
        prefix + "qkv_w": (gaussian(2, (D, 3, HEADS, HEAD)) * D ** -0.5).astype(jnp.bfloat16),
        prefix + "qkv_b": (0.2 * gaussian(3, (3, HEADS, HEAD))).astype(jnp.bfloat16),
        prefix + "out_w": (gaussian(4, (HEADS, HEAD, D)) * HIDDEN ** -0.5).astype(jnp.bfloat16),
        prefix + "out_b": (0.2 * gaussian(5, (D,))).astype(jnp.bfloat16),
        prefix + "norm2_gain": (1.0 + 0.2 * gaussian(6, (D,))).astype(jnp.bfloat16),
        prefix + "norm2_bias": (0.2 * gaussian(7, (D,))).astype(jnp.bfloat16),
        prefix + "up_w": (gaussian(8, (D, FF)) * D ** -0.5).astype(jnp.bfloat16),
        prefix + "up_b": (0.2 * gaussian(9, (FF,))).astype(jnp.bfloat16),
        prefix + "down_w": (gaussian(10, (FF, D)) * FF ** -0.5).astype(jnp.bfloat16),
        prefix + "down_b": (0.2 * gaussian(11, (D,))).astype(jnp.bfloat16),
    }


def setup_inputs(seed: int = 0) -> dict:
    key_list = jax.random.split(jax.random.key(seed), 26)
    result = {
        "act_in": jax.random.normal(key_list[0], (BATCH, SEQ, D), jnp.float32).astype(jnp.bfloat16),
        "grad_out": jax.random.normal(key_list[1], (BATCH, SEQ, D), jnp.float32).astype(jnp.bfloat16),
    }
    result.update(draw_layer(key_list[2:14], "l1_"))
    result.update(draw_layer(key_list[14:26], "l2_"))
    return result


def to_bf16(values):
    return values.astype(jnp.bfloat16).astype(jnp.float32)


def layer_norm(x_f, gain, shift):
    row_mean = jnp.mean(x_f, axis=-1, keepdims=True)
    centred = x_f - row_mean
    row_var = jnp.mean(centred * centred, axis=-1, keepdims=True)
    return centred * lax.rsqrt(row_var + 1e-5) * gain + shift


def attend(q_blk, k_blk, v_blk, allowed):
    scores = jnp.einsum("bqhe,bkhe->bhqk", q_blk, k_blk) * HEAD ** -0.5
    scores = jnp.where(allowed, scores, -1e30)
    attn_probs = to_bf16(jax.nn.softmax(scores, axis=-1))
    return jnp.einsum("bhqk,bkhe->bqhe", attn_probs, v_blk)


def dense_attention(q_all, k_all, v_all):
    q_blocks = jnp.moveaxis(q_all.reshape(BATCH, BLOCKS, SEQ_DEV, HEADS, HEAD), 1, 0)
    key_pos = jnp.arange(SEQ)

    def one_block(blk_args):
        blk_index, q_blk = blk_args
        q_pos = blk_index * SEQ_DEV + jnp.arange(SEQ_DEV)
        return attend(q_blk, k_all, v_all, key_pos[None, :] <= q_pos[:, None])

    blk_out = lax.map(jax.checkpoint(one_block), (jnp.arange(BLOCKS), q_blocks))
    return jnp.moveaxis(blk_out, 0, 1).reshape(BATCH, SEQ, HEADS, HEAD)


def band_attention(q_all, k_all, v_all):
    q_blocks = jnp.moveaxis(q_all.reshape(BATCH, BLOCKS, SEQ_DEV, HEADS, HEAD), 1, 0)
    zero_pad = jnp.zeros((BATCH, WINDOW, HEADS, HEAD), q_all.dtype)
    k_pad = jnp.concatenate([zero_pad, k_all], axis=1)
    v_pad = jnp.concatenate([zero_pad, v_all], axis=1)
    span_len = SEQ_DEV + WINDOW
    pos_diff = (jnp.arange(SEQ_DEV) + WINDOW)[:, None] - jnp.arange(span_len)[None, :]

    def one_block(blk_args):
        blk_index, q_blk = blk_args
        blk_start = blk_index * SEQ_DEV
        k_blk = lax.dynamic_slice_in_dim(k_pad, blk_start, span_len, axis=1)
        v_blk = lax.dynamic_slice_in_dim(v_pad, blk_start, span_len, axis=1)
        key_pos = blk_start - WINDOW + jnp.arange(span_len)
        allowed = (pos_diff >= 0) & (pos_diff < WINDOW) & (key_pos[None, :] >= 0)
        return attend(q_blk, k_blk, v_blk, allowed)

    blk_out = lax.map(jax.checkpoint(one_block), (jnp.arange(BLOCKS), q_blocks))
    return jnp.moveaxis(blk_out, 0, 1).reshape(BATCH, SEQ, HEADS, HEAD)


def gpt_layer(x_in, params, banded):
    (n1_gain, n1_bias, qkv_w, qkv_b, out_w, out_b, n2_gain, n2_bias, up_w, up_b, down_w, down_b) = params
    x_f = x_in.astype(jnp.float32)
    hid_one = to_bf16(layer_norm(x_f, n1_gain, n1_bias))
    qkv_all = to_bf16(jnp.einsum("bsd,dthe->tbshe", hid_one, qkv_w) + qkv_b[:, None, None])
    attend_fn = band_attention if banded else dense_attention
    attn_out = to_bf16(attend_fn(qkv_all[0], qkv_all[1], qkv_all[2]))
    x_mid = to_bf16(x_f + jnp.einsum("bshe,hed->bsd", attn_out, out_w) + out_b)
    hid_two = to_bf16(layer_norm(x_mid, n2_gain, n2_bias))
    up_act = to_bf16(jax.nn.gelu(jnp.einsum("bsd,df->bsf", hid_two, up_w) + up_b, approximate=True))
    return (x_mid + jnp.einsum("bsf,fd->bsd", up_act, down_w) + down_b).astype(jnp.bfloat16)


def reference(act_in, grad_out, l1_norm1_gain, l1_norm1_bias, l1_qkv_w, l1_qkv_b, l1_out_w, l1_out_b, l1_norm2_gain, l1_norm2_bias, l1_up_w, l1_up_b, l1_down_w, l1_down_b, l2_norm1_gain, l2_norm1_bias, l2_qkv_w, l2_qkv_b, l2_out_w, l2_out_b, l2_norm2_gain, l2_norm2_bias, l2_up_w, l2_up_b, l2_down_w, l2_down_b):
    weights = [l1_norm1_gain, l1_norm1_bias, l1_qkv_w, l1_qkv_b, l1_out_w, l1_out_b, l1_norm2_gain, l1_norm2_bias, l1_up_w, l1_up_b, l1_down_w, l1_down_b, l2_norm1_gain, l2_norm1_bias, l2_qkv_w, l2_qkv_b, l2_out_w, l2_out_b, l2_norm2_gain, l2_norm2_bias, l2_up_w, l2_up_b, l2_down_w, l2_down_b]
    params = [weight.astype(jnp.float32) for weight in weights]

    def forward(x_in, flat_params):
        return gpt_layer(gpt_layer(x_in, flat_params[:12], False), flat_params[12:], True)

    act_out, pullback = jax.vjp(forward, act_in, params)
    grad_in, weight_grads = pullback(grad_out)
    return (act_out, grad_in, weight_grads[0], weight_grads[1], weight_grads[2], weight_grads[3], weight_grads[4], weight_grads[5], weight_grads[6], weight_grads[7], weight_grads[8], weight_grads[9], weight_grads[10], weight_grads[11], weight_grads[12], weight_grads[13], weight_grads[14], weight_grads[15], weight_grads[16], weight_grads[17], weight_grads[18], weight_grads[19], weight_grads[20], weight_grads[21], weight_grads[22], weight_grads[23])
```

```python
import jax
import jax.numpy as jnp
from jax import lax
from jax.experimental import pallas as pl
from jax.experimental.layout import Layout, with_layout_constraint
from jax.experimental.pallas import tpu as pltpu
from jax.sharding import PartitionSpec as P

SEQ_AXIS = "cp"
WINDOW = 256
LN_EPS = 1e-5
HEADS = 16
HEAD = 96
GROUPS = 2
LOG2E = 1.4426950408889634
MASKED = -1e30
CORE_PAIRS = tuple((i, i ^ 1) for i in range(8))
X_PAIRS = tuple((i, i ^ 2) for i in range(8))
Y_PAIRS = tuple((i, i ^ 4) for i in range(8))


def swap_core(a):
    return lax.ppermute(a, SEQ_AXIS, CORE_PAIRS)


def swap_x(a):
    return lax.ppermute(a, SEQ_AXIS, X_PAIRS)


def swap_y(a):
    return lax.ppermute(a, SEQ_AXIS, Y_PAIRS)


def place_kernel(dest_ref, own_ref, other_ref, out_ref):
    @pl.when(pl.program_id(0) == 0)
    def _():
        out_ref[...] = own_ref[...].astype(jnp.float32)

    @pl.when(pl.program_id(0) == 1)
    def _():
        out_ref[...] = other_ref[...].astype(jnp.float32)


def place_blocks(own, other, dest):
    half_rows, n = own.shape
    rows = half_rows // 8
    spec = pltpu.PrefetchScalarGridSpec(
        num_scalar_prefetch=1, grid=(2, 8),
        in_specs=[pl.BlockSpec((rows, n), lambda k, i, dest_ref: (jnp.where(k == 0, i, 7), 0)),
                  pl.BlockSpec((rows, n), lambda k, i, dest_ref: (jnp.where(k == 0, 0, i), 0))],
        out_specs=pl.BlockSpec((rows, n), lambda k, i, dest_ref: (dest_ref[k * 8 + i], 0)))
    return pl.pallas_call(
        place_kernel, grid_spec=spec, out_shape=jax.ShapeDtypeStruct((2 * half_rows, n), jnp.float32),
        cost_estimate=pl.CostEstimate(flops=60 * half_rows * n, bytes_accessed=half_rows * n * 12, transcendentals=0),
        compiler_params=pltpu.CompilerParams(dimension_semantics=("arbitrary", "arbitrary")),
        name="place_blocks")(dest, own, other)


def tie(*values):
    return lax.optimization_barrier(values)


def product_task(left, right, bits, left_axis):
    core, x, y, dest = bits
    m = left.shape[left_axis]
    half, quarter, eighth, part = m // 2, m // 4, m // 8, m // 16

    def rows(a, start, count):
        return lax.dynamic_slice_in_dim(a, start, count, 0)

    def product(which):
        chosen = lax.dynamic_slice_in_dim(left, which * half, half, left_axis)
        return lax.dot_general(chosen, right, (((1 - left_axis,), (0,)), ((), ())), preferred_element_type=jnp.float32)

    to_partner = product(1 - core).astype(jnp.bfloat16)
    (from_partner,) = yield ((swap_core, to_partner),)
    kept = product(core) + from_partner.astype(jnp.float32)

    def outgoing(base, first):
        return rows(kept, base + (1 - first) * eighth, eighth).astype(jnp.bfloat16)

    got_a, got_b = yield ((swap_x, outgoing(0, x)), (swap_y, outgoing(quarter, y)))

    def twice(base, first, got, which):
        return rows(kept, base + first * eighth + which * part, part) + rows(got, which * part, part).astype(jnp.float32)

    more_a, more_b = yield ((swap_y, twice(0, x, got_a, 1 - y).astype(jnp.bfloat16)),
                            (swap_x, twice(quarter, y, got_b, 1 - x).astype(jnp.bfloat16)))
    own_a = (twice(0, x, got_a, y) + more_a.astype(jnp.float32)).astype(jnp.bfloat16)
    own_b = (twice(quarter, y, got_b, x) + more_b.astype(jnp.float32)).astype(jnp.bfloat16)
    other_a, other_b = yield ((swap_y, own_a), (swap_x, own_b))
    pair_a = jnp.concatenate([own_a, other_a], 0)
    pair_b = jnp.concatenate([own_b, other_b], 0)
    far_a, far_b = yield ((swap_x, pair_a), (swap_y, pair_b))
    own_half = jnp.concatenate([pair_a, far_a, pair_b, far_b], 0)
    (other_half,) = yield ((swap_core, own_half),)
    return own_half, other_half


def scatter_task(keep, send, bits):
    _, x, y, _ = bits
    got = yield tuple((swap_core, part) for part in send)
    own = [(part + other.astype(jnp.float32)).reshape(2, 2, *part.shape[1:]) for part, other in zip(keep, got)]

    def pick(a, axis, index):
        return lax.dynamic_index_in_dim(a, index, axis, keepdims=False)

    got = yield ((swap_x, pick(own[0], 1, 1 - x).astype(jnp.bfloat16)), (swap_y, pick(own[1], 0, 1 - y).astype(jnp.bfloat16)))
    own = [pick(own[0], 1, x) + got[0].astype(jnp.float32), pick(own[1], 0, y) + got[1].astype(jnp.float32)]
    got = yield ((swap_y, pick(own[0], 0, 1 - y).astype(jnp.bfloat16)), (swap_x, pick(own[1], 0, 1 - x).astype(jnp.bfloat16)))
    return [pick(own[0], 0, y) + got[0].astype(jnp.float32), pick(own[1], 0, x) + got[1].astype(jnp.float32)]


def vector_task(vectors):
    flat = jnp.concatenate([v.reshape(-1) for v in vectors])
    flat = jnp.pad(flat, (0, -flat.size % 1024)).reshape(-1, 1024)
    for swap in (swap_core, swap_x, swap_y):
        (got,) = yield ((swap, flat),)
        flat = flat + got
    return flat.reshape(-1)


class Exchanges:
    def __init__(self, bits):
        self.bits = bits
        self.running = []
        self.results = {}
        self.fillers = []
        self.filled = {}

    def add(self, name, task):
        self.running.append([name, task, None])

    def product(self, name, left, right, left_axis):
        self.add(name, product_task(left, right, self.bits, left_axis))

    def fill(self, name, compute):
        self.fillers.append((name, compute))

    def slot(self, main, fill=0):
        names = list(self.filled)
        main, arrived, filled = tie(main, [pending for _, _, pending in self.running], [self.filled[name] for name in names])
        self.filled.update(zip(names, filled))
        still, outgoing = [], []
        for (name, task, _), got in zip(self.running, arrived):
            try:
                sends = next(task) if got is None else task.send(got)
            except StopIteration as finished:
                self.results[name] = finished.value
                if isinstance(finished.value, tuple):
                    self.fill(name, lambda halves=finished.value: place_blocks(*halves, self.bits[3]))
                continue
            still.append([name, task, [swap for swap, _ in sends]])
            outgoing.append([value for _, value in sends])
        main, outgoing = tie(main, outgoing)
        for entry, values in zip(still, outgoing):
            entry[2] = tuple(swap(value) for swap, value in zip(entry[2], values))
        self.running = still
        for name, compute in self.fillers[:fill]:
            self.filled[name] = compute()
        self.fillers = self.fillers[fill:]
        return main

    def finish(self, main, fill):
        while self.running:
            main = self.slot(main, fill)
        for name, compute in self.fillers:
            self.filled[name] = compute()
        return main

    def vectors(self, name, shapes):
        flat, start, result = self.results[name], 0, []
        for v in shapes:
            result.append(flat[start:start + v.size].reshape(v.shape))
            start += v.size
        return result


def device_bits(my_rank):
    core, x, y = my_rank % 2, (my_rank // 2) % 2, my_rank // 4
    dest = []
    for half_core in (core, 1 - core):
        for p in range(2):
            for q in range(2):
                dest.append(half_core * 8 + jnp.bitwise_xor(x, p) * 2 + jnp.bitwise_xor(y, q))
        for p in range(2):
            for q in range(2):
                dest.append(half_core * 8 + 4 + jnp.bitwise_xor(y, p) * 2 + jnp.bitwise_xor(x, q))
    return core, x, y, jnp.stack(dest).astype(jnp.int32)


def layer_norm(x_f, gain, shift):
    row_mean = jnp.mean(x_f, axis=-1, keepdims=True)
    centred = x_f - row_mean
    row_var = jnp.mean(centred * centred, axis=-1, keepdims=True)
    return centred * lax.rsqrt(row_var + LN_EPS) * gain + shift


def gelu_tanh(pre_act):
    return jax.nn.gelu(pre_act, approximate=True)


def dot_tn(a, b):
    return lax.dot_general(a, b, (((0,), (0,)), ((), ())), preferred_element_type=jnp.float32)


def dot_nn(a, b):
    return lax.dot_general(a, b, (((1,), (0,)), ((), ())), preferred_element_type=jnp.float32)


def dot_nt(a, b):
    return lax.dot_general(a, b, (((1,), (1,)), ((), ())), preferred_element_type=jnp.float32)


def query_minus_key(n_keys, n_queries):
    return lax.broadcasted_iota(jnp.int32, (n_keys, n_queries), 1) - lax.broadcasted_iota(jnp.int32, (n_keys, n_queries), 0)


def score_factor(head):
    return head ** -0.5 * LOG2E


def dense_forward_kernel(rank_ref, q_ref, k_ref, v_ref, o_ref, lse_ref):
    rank = rank_ref[0]
    q = q_ref[...]
    head, block = q.shape
    diff = query_minus_key(block, block)

    def step(j, carry):
        top, total, acc = carry
        scores = dot_tn(k_ref[j], q) * score_factor(head)
        scores = jnp.where(diff >= jnp.where(j == rank, 0, -block), scores, MASKED)
        new_top = jnp.maximum(top, jnp.max(scores, axis=0, keepdims=True))
        shrink = jnp.exp2(top - new_top)
        probs = jnp.exp2(scores - new_top)
        total = total * shrink + jnp.sum(probs, axis=0, keepdims=True)
        acc = acc * shrink + dot_nn(v_ref[j], probs.astype(jnp.bfloat16))
        return new_top, total, acc

    start = (jnp.full((1, block), MASKED, jnp.float32), jnp.zeros((1, block), jnp.float32), jnp.zeros((head, block), jnp.float32))
    top, total, acc = lax.fori_loop(0, rank + 1, step, start)
    o_ref[...] = (acc / total).astype(jnp.bfloat16)
    lse_ref[0] = top + jnp.log2(total)


def dense_backward_kernel(rank_ref, q_ref, k_ref, v_ref, o_ref, do_ref, lse_ref,
                          dq_ref, dk_keep_ref, dv_keep_ref, dk_send_ref, dv_send_ref):
    rank = rank_ref[0]
    core = lax.rem(rank, 2)
    q, d_out = q_ref[...], do_ref[...]
    head, block = q.shape
    scale = head ** -0.5
    diff = query_minus_key(block, block)
    delta = jnp.sum(o_ref[...].astype(jnp.float32) * d_out.astype(jnp.float32), axis=0, keepdims=True)
    lse = lse_ref[0]
    dq_ref[...] = jnp.zeros_like(dq_ref)

    def block_grads(j):
        k, v = k_ref[j], v_ref[j]
        scores = dot_tn(k, q) * score_factor(head)
        scores = jnp.where(diff >= jnp.where(j == rank, 0, -block), scores, MASKED)
        probs = jnp.exp2(scores - lse)
        d_scores = (probs * (dot_tn(v, d_out) - delta)).astype(jnp.bfloat16)
        dq_ref[...] += dot_nn(k, d_scores) * scale
        return dot_nt(q, d_scores) * scale, dot_nt(d_out, probs.astype(jnp.bfloat16))

    def fill(pair, j, dk_ref, dv_ref):
        @pl.when(j <= rank)
        def _():
            dk, dv = block_grads(j)
            dk_ref[pair] = dk.astype(dk_ref.dtype)
            dv_ref[pair] = dv.astype(dv_ref.dtype)

        @pl.when(j > rank)
        def _():
            dk_ref[pair] = jnp.zeros(dk_ref.shape[1:], dk_ref.dtype)
            dv_ref[pair] = jnp.zeros(dv_ref.shape[1:], dv_ref.dtype)

    def step(pair, carry):
        fill(pair, 2 * pair + core, dk_keep_ref, dv_keep_ref)
        fill(pair, 2 * pair + 1 - core, dk_send_ref, dv_send_ref)
        return carry

    lax.fori_loop(0, 4, step, 0)


def band_mask(rank, half):
    diff = query_minus_key(2 * WINDOW, WINDOW)
    allowed = (diff < 0) & (diff >= -WINDOW)
    if half == 0:
        first_key = jnp.where(rank == 0, WINDOW, 0)
        allowed = allowed & (lax.broadcasted_iota(jnp.int32, (2 * WINDOW, WINDOW), 0) >= first_key)
    return allowed


def band_forward_kernel(rank_ref, q_ref, k_ref, v_ref, o_ref, lse_ref):
    head = q_ref.shape[0]
    for half in range(2):
        at_q, at_k = pl.ds(half * WINDOW, WINDOW), pl.ds(half * WINDOW, 2 * WINDOW)
        scores = dot_tn(k_ref[:, at_k], q_ref[:, at_q]) * score_factor(head)
        scores = jnp.where(band_mask(rank_ref[0], half), scores, MASKED)
        top = jnp.max(scores, axis=0, keepdims=True)
        probs = jnp.exp2(scores - top)
        total = jnp.sum(probs, axis=0, keepdims=True)
        out = dot_nn(v_ref[:, at_k], probs.astype(jnp.bfloat16))
        o_ref[:, at_q] = (out / total).astype(jnp.bfloat16)
        lse_ref[0, :, at_q] = top + jnp.log2(total)


def band_backward_kernel(rank_ref, q_ref, k_ref, v_ref, o_ref, do_ref, lse_ref, dq_ref, dk_ref, dv_ref):
    head = q_ref.shape[0]
    scale = head ** -0.5
    for half in range(2):
        at_q, at_k = pl.ds(half * WINDOW, WINDOW), pl.ds(half * WINDOW, 2 * WINDOW)
        q, d_out, k, v = q_ref[:, at_q], do_ref[:, at_q], k_ref[:, at_k], v_ref[:, at_k]
        delta = jnp.sum(o_ref[:, at_q].astype(jnp.float32) * d_out.astype(jnp.float32), axis=0, keepdims=True)
        scores = dot_tn(k, q) * score_factor(head)
        scores = jnp.where(band_mask(rank_ref[0], half), scores, MASKED)
        probs = jnp.exp2(scores - lse_ref[0, :, at_q])
        d_scores = (probs * (dot_tn(v, d_out) - delta)).astype(jnp.bfloat16)
        dq_ref[:, at_q] = dot_nn(k, d_scores) * scale
        for out_ref, value in ((dk_ref, dot_nt(q, d_scores) * scale), (dv_ref, dot_nt(d_out, probs.astype(jnp.bfloat16)))):
            if half == 0:
                out_ref[:, pl.ds(0, 2 * WINDOW)] = value
            else:
                out_ref[:, pl.ds(WINDOW, WINDOW)] += value[:, :WINDOW]
                out_ref[:, pl.ds(2 * WINDOW, WINDOW)] = value[:, WINDOW:]


def head_call(kernel, name, rank, heads, operands, out_shapes, flops):
    def spec(shape, offset):
        if shape[-2] == 1:
            return pl.BlockSpec((1,) + shape[1:], lambda h, rank_ref: (h + offset, 0, 0))
        if len(shape) == 2:
            return pl.BlockSpec((HEAD, shape[1]), lambda h, rank_ref: (h + offset, 0))
        return pl.BlockSpec((shape[0], HEAD, shape[2]), lambda h, rank_ref: (0, h + offset, 0))

    grid_spec = pltpu.PrefetchScalarGridSpec(
        num_scalar_prefetch=1, grid=(heads,),
        in_specs=[spec(a.shape, offset) for a, offset in operands],
        out_specs=[spec(s.shape, 0) for s in out_shapes])
    return pl.pallas_call(
        kernel, grid_spec=grid_spec, out_shape=out_shapes,
        cost_estimate=pl.CostEstimate(flops=flops, bytes_accessed=sum(a.size * 2 for a, _ in operands), transcendentals=0),
        compiler_params=pltpu.CompilerParams(dimension_semantics=("arbitrary",)), name=name)(rank, *[a for a, _ in operands])


def shape_of(*shape, dtype=jnp.float32):
    return jax.ShapeDtypeStruct(shape, dtype)


def row_major(a):
    return with_layout_constraint(a, Layout(major_to_minor=tuple(range(a.ndim))))


def layer_forward(x_in, layer_wts, banded, rank, n_dev):
    (n1_gain, n1_bias, qkv_w, qkv_b, out_w, out_b, n2_gain, n2_bias, up_w, up_b, down_w, down_b) = layer_wts
    x_f = x_in.astype(jnp.float32)
    hid_one = layer_norm(x_f, n1_gain.astype(jnp.float32), n1_bias.astype(jnp.float32)).astype(jnp.bfloat16)
    hidden = out_w.shape[0] * out_w.shape[1]
    qkv_w2 = qkv_w.reshape(-1, 3 * hidden)

    def project(start, count):
        rows = lax.dot_general(qkv_w2[:, start:start + count], hid_one, (((0,), (1,)), ((), ())), preferred_element_type=jnp.float32)
        return (rows + qkv_b.reshape(-1)[start:start + count, None].astype(jnp.float32)).astype(jnp.bfloat16)

    if banded:
        qkv_t = project(0, 3 * hidden)
        q_t, kv_t = qkv_t[:hidden], qkv_t[hidden:]
        block = q_t.shape[1]
        to_next = [(source, source + 1) for source in range(n_dev - 1)]
        prev_tail = lax.ppermute(kv_t[:, block - WINDOW:], SEQ_AXIS, to_next)
        context = jnp.concatenate([prev_tail, kv_t], axis=1)
        attn_t, lse = head_call(band_forward_kernel, "band_forward", rank, HEADS,
                                [(q_t, 0), (context, 0), (context, HEADS)],
                                [shape_of(hidden, block, dtype=jnp.bfloat16), shape_of(HEADS, 1, block)], 4_000_000_000)
    else:
        q_t, kv_t = project(0, hidden), project(hidden, 2 * hidden)
        context = []
        size = hidden // GROUPS
        for g in range(GROUPS):
            part = jnp.concatenate([kv_t[g * size:(g + 1) * size], kv_t[hidden + g * size:hidden + (g + 1) * size]], 0)
            part = row_major(lax.all_gather(row_major(part), SEQ_AXIS))
            context.append((part, part))
        outs = [head_call(dense_forward_kernel, "dense_forward", rank, HEADS // GROUPS,
                          [(q_t, g * (HEADS // GROUPS)), (k_all, 0), (v_all, HEADS // GROUPS)],
                          [shape_of(size, q_t.shape[1], dtype=jnp.bfloat16), shape_of(HEADS // GROUPS, 1, q_t.shape[1])], 25_000_000_000)
                for g, (k_all, v_all) in enumerate(context)]
        attn_t, lse = jnp.concatenate([o for o, _ in outs], 0), [part for _, part in outs]
    x_mid = (x_f + lax.dot_general(attn_t, out_w.reshape(hidden, -1), (((0,), (0,)), ((), ())), preferred_element_type=jnp.float32)
             + out_b.astype(jnp.float32)).astype(jnp.bfloat16)
    mid_f = x_mid.astype(jnp.float32)
    hid_two = layer_norm(mid_f, n2_gain.astype(jnp.float32), n2_bias.astype(jnp.float32)).astype(jnp.bfloat16)
    up_pre = dot_nn(hid_two, up_w) + up_b.astype(jnp.float32)
    up_act = gelu_tanh(up_pre).astype(jnp.bfloat16)

    def output():
        return (mid_f + dot_nn(up_act, down_w) + down_b.astype(jnp.float32)).astype(jnp.bfloat16)

    return output, (x_f, hid_one, q_t, context, lse, attn_t, mid_f, hid_two, up_pre, up_act)


def layer_backward(d_out, layer_wts, saved_acts, banded, rank, n_dev, comm, tag):
    n1_gain, n1_bias, qkv_w, out_w = layer_wts[0], layer_wts[1], layer_wts[2], layer_wts[4]
    n2_gain, n2_bias, up_w, down_w = layer_wts[6], layer_wts[7], layer_wts[8], layer_wts[10]
    (x_f, hid_one, q_t, context, lse, attn_t, mid_f, hid_two, up_pre, up_act) = saved_acts
    hidden, block = q_t.shape
    d_out16 = d_out.astype(jnp.bfloat16)
    comm.product(tag + "down_w", up_act, d_out16, 1)
    d_out, d_out16 = comm.slot((d_out, d_out16))
    g_down_b = jnp.sum(d_out, axis=0)
    d_act = dot_nt(d_out16, down_w)
    d_up = jax.vjp(gelu_tanh, up_pre)[1](d_act)[0]
    d_up16 = d_up.astype(jnp.bfloat16)
    g_up_b = jnp.sum(d_up, axis=0)
    comm.product(tag + "up_w", hid_two, d_up16, 1)
    (d_up16,) = comm.slot((d_up16,))
    d_hid_two = dot_nt(d_up16, up_w)
    norm2_pull = jax.vjp(layer_norm, mid_f, n2_gain.astype(jnp.float32), n2_bias.astype(jnp.float32))[1]
    d_mid_norm, g_n2_gain, g_n2_bias = norm2_pull(d_hid_two)
    d_mid = d_out + d_mid_norm
    d_mid16 = d_mid.astype(jnp.bfloat16)
    comm.product(tag + "out_w", attn_t, d_mid16, 0)
    d_mid, d_mid16 = comm.slot((d_mid, d_mid16))
    g_out_b = jnp.sum(d_mid, axis=0)
    d_attn_t = dot_nt(out_w.reshape(hidden, -1), d_mid16).astype(jnp.bfloat16)
    if banded:
        d_q, d_k, d_v = head_call(band_backward_kernel, "band_backward", rank, HEADS,
                                  [(q_t, 0), (context, 0), (context, HEADS), (attn_t, 0), (d_attn_t, 0), (lse, 0)],
                                  [shape_of(hidden, block), shape_of(hidden, block + WINDOW), shape_of(hidden, block + WINDOW)],
                                  10_000_000_000)
        to_prev = [(source + 1, source) for source in range(n_dev - 1)]
        tails = jnp.concatenate([d_k[:, :WINDOW], d_v[:, :WINDOW]], 0).astype(jnp.bfloat16)
        from_next = lax.ppermute(tails, SEQ_AXIS, to_prev)
        d_q, d_k, d_v, from_next = comm.slot((d_q, d_k, d_v, from_next))
        from_next = jnp.pad(from_next.astype(jnp.float32), ((0, 0), (block - WINDOW, 0)))
        d_k = d_k[:, WINDOW:] + from_next[:hidden]
        d_v = d_v[:, WINDOW:] + from_next[hidden:]
    else:
        heads, size = HEADS // GROUPS, hidden // GROUPS
        d_q, d_k, d_v = [], [], []
        for g, (k_all, v_all) in enumerate(context):
            half = [shape_of(4, size, block, dtype=dtype) for dtype in (jnp.float32, jnp.float32, jnp.bfloat16, jnp.bfloat16)]
            dq_g, dk_keep, dv_keep, dk_send, dv_send = head_call(
                dense_backward_kernel, "dense_backward", rank, heads,
                [(q_t, g * heads), (k_all, 0), (v_all, heads), (attn_t, g * heads), (d_attn_t, g * heads), (lse[g], 0)],
                [shape_of(size, block)] + half, 60_000_000_000)
            d_q.append(dq_g)
            comm.add("d_kv%d" % g, scatter_task((dk_keep, dv_keep), (dk_send, dv_send), comm.bits))
            (d_attn_t, d_q) = comm.slot((d_attn_t, d_q))
        for _ in range(3):
            (d_q,) = comm.slot((d_q,), fill=2)
        for g in range(GROUPS):
            dk_g, dv_g = comm.results["d_kv%d" % g]
            d_k.append(dk_g)
            d_v.append(dv_g)
        d_q, d_k, d_v = (jnp.concatenate(parts, 0) for parts in (d_q, d_k, d_v))
    d_qkv = jnp.concatenate([d_q, d_k, d_v], 0)
    g_qkv_b = jnp.sum(d_qkv, axis=1)
    d_qkv16 = d_qkv.astype(jnp.bfloat16)
    comm.product(tag + "qkv_w", d_qkv16, hid_one, 0)
    d_mid, d_qkv16 = comm.slot((d_mid, d_qkv16))
    d_hid_one = lax.dot_general(d_qkv16, qkv_w.reshape(-1, 3 * hidden), (((0,), (1,)), ((), ())), preferred_element_type=jnp.float32)
    norm1_pull = jax.vjp(layer_norm, x_f, n1_gain.astype(jnp.float32), n1_bias.astype(jnp.float32))[1]
    d_in_norm, g_n1_gain, g_n1_bias = norm1_pull(d_hid_one)
    small = (g_n1_gain, g_n1_bias, g_qkv_b, g_out_b, g_n2_gain, g_n2_bias, g_up_b, g_down_b)
    comm.add(tag + "small", vector_task(small))
    return d_mid + d_in_norm, small


def layer_gradients(comm, tag, small, layer_wts):
    qkv_w, out_w = layer_wts[2], layer_wts[4]
    g_n1_gain, g_n1_bias, g_qkv_b, g_out_b, g_n2_gain, g_n2_bias, g_up_b, g_down_b = comm.vectors(tag + "small", small)
    g_qkv_w = comm.filled[tag + "qkv_w"].reshape(qkv_w.shape[1:] + qkv_w.shape[:1]).transpose(3, 0, 1, 2)
    g_out_w = comm.filled[tag + "out_w"].reshape(out_w.shape)
    g_qkv_b = g_qkv_b.reshape(qkv_w.shape[1:])
    return (g_n1_gain, g_n1_bias, g_qkv_w, g_qkv_b, g_out_w, g_out_b, g_n2_gain, g_n2_bias,
            comm.filled[tag + "up_w"], g_up_b, comm.filled[tag + "down_w"], g_down_b)


def solution(mesh):
    n_dev = mesh.shape[SEQ_AXIS]

    def sharded_step(act_in, grad_out, *weights):
        my_rank = lax.axis_index(SEQ_AXIS)
        bits = device_bits(my_rank)
        rank = my_rank.reshape(1).astype(jnp.int32)
        act_mid, saved_one = layer_forward(act_in[0], weights[:12], False, rank, n_dev)
        act_out, saved_two = layer_forward(act_mid(), weights[12:], True, rank, n_dev)
        comm = Exchanges(bits)
        comm.fill("y", act_out)
        d_mid, small_two = layer_backward(grad_out[0].astype(jnp.float32), weights[12:], saved_two, True, rank, n_dev, comm, "2")
        d_in, small_one = layer_backward(d_mid, weights[:12], saved_one, False, rank, n_dev, comm, "1")
        (d_in,) = comm.finish((d_in,), 2)
        grads_one = layer_gradients(comm, "1", small_one, weights[:12])
        grads_two = layer_gradients(comm, "2", small_two, weights[12:])
        return (comm.filled["y"][None], d_in.astype(jnp.bfloat16)[None]) + grads_one + grads_two

    seq_spec = P(None, SEQ_AXIS, None)
    specs_in = (seq_spec, seq_spec) + (P(),) * 24
    specs_out = (seq_spec, seq_spec) + (P(),) * 24
    return jax.shard_map(sharded_step, mesh=mesh, in_specs=specs_in, out_specs=specs_out, check_vma=False)
```

```python
import functools

import jax
import jax.numpy as jnp
from jax import lax
from jax.experimental import pallas as pl
from jax.experimental.layout import Layout, with_layout_constraint
from jax.experimental.pallas import tpu as pltpu
from jax.sharding import PartitionSpec as P

SEQ_AXIS = "cp"
WINDOW = 256
LN_EPS = 1e-5
HEADS = 16
HEAD = 96
GROUPS = 4
LOG2E = 1.4426950408889634
MASKED = -1e30
CORE_PAIRS = tuple((i, i ^ 1) for i in range(8))
X_PAIRS = tuple((i, i ^ 2) for i in range(8))
Y_PAIRS = tuple((i, i ^ 4) for i in range(8))


def swap_core(a):
    return lax.ppermute(a, SEQ_AXIS, CORE_PAIRS)


def swap_x(a):
    return lax.ppermute(a, SEQ_AXIS, X_PAIRS)


def swap_y(a):
    return lax.ppermute(a, SEQ_AXIS, Y_PAIRS)


def row_major(a):
    return with_layout_constraint(a, Layout(major_to_minor=tuple(range(a.ndim))))


def place_kernel(gathered_ref, *refs):
    refs[-1][...] = gathered_ref[0].astype(jnp.float32)


def place_blocks(gathered, into, total_rows, first_row):
    n = gathered.shape[2]
    rows = gathered.shape[1] // 2
    first = first_row // rows

    def target(device, part):
        core, x, y = device % 2, (device // 2) % 2, device // 4
        return first + core * 8 + part * 4 + jnp.where(part == 0, x * 2 + y, y * 2 + x), 0

    operands = [gathered] if into is None else [gathered, into]
    return pl.pallas_call(
        place_kernel, grid=(8, 2),
        in_specs=[pl.BlockSpec((1, rows, n), lambda device, part: (device, part, 0))] + [pl.BlockSpec(memory_space=pl.ANY)] * (len(operands) - 1),
        out_specs=pl.BlockSpec((rows, n), target),
        out_shape=jax.ShapeDtypeStruct((total_rows, n), jnp.float32),
        input_output_aliases={} if into is None else {1: 0},
        cost_estimate=pl.CostEstimate(flops=60 * gathered.size // 2, bytes_accessed=gathered.size * 6, transcendentals=0),
        compiler_params=pltpu.CompilerParams(dimension_semantics=("arbitrary", "arbitrary")),
        name="place_blocks")(*operands)


def tie(*values):
    return lax.optimization_barrier(values)


def kept_kernel(left_axis, index_ref, left_ref, right_ref, got_ref, *out_refs):
    value = lax.dot_general(left_ref[...], right_ref[...], (((1 - left_axis,), (0,)), ((), ())), preferred_element_type=jnp.float32)
    value = value + got_ref[...].astype(jnp.float32)
    for k, out_ref in enumerate(out_refs):
        @pl.when(pl.program_id(0) // 2 == k)
        def _(out_ref=out_ref):
            out_ref[...] = value.astype(out_ref.dtype)


def kept_product(left, right, got, bits, left_axis):
    core, x, y = bits
    tokens, n = right.shape
    part = left.shape[left_axis] // 16
    index = jnp.stack([(1 - x) * 2, (1 - x) * 2 + 1, 4 + (1 - y) * 2, 5 + (1 - y) * 2, x * 2, x * 2 + 1, 4 + y * 2, 5 + y * 2])
    index = jnp.concatenate([index, index + core * 8]).astype(jnp.int32)
    if left_axis == 0:
        left_spec = pl.BlockSpec((part, tokens), lambda i, index_ref: (index_ref[8 + i], 0))
    else:
        left_spec = pl.BlockSpec((tokens, part), lambda i, index_ref: (0, index_ref[8 + i]))

    def out_spec(k):
        return pl.BlockSpec((part, n), lambda i, index_ref: (jnp.clip(i - 2 * k, 0, 1), 0))

    grid_spec = pltpu.PrefetchScalarGridSpec(
        num_scalar_prefetch=1, grid=(8,),
        in_specs=[left_spec, pl.BlockSpec((tokens, n), lambda i, index_ref: (0, 0)), pl.BlockSpec((part, n), lambda i, index_ref: (index_ref[i], 0))],
        out_specs=[out_spec(k) for k in range(4)])
    dtypes = (jnp.bfloat16, jnp.bfloat16, jnp.float32, jnp.float32)
    return pl.pallas_call(
        functools.partial(kept_kernel, left_axis), grid_spec=grid_spec,
        out_shape=[jax.ShapeDtypeStruct((2 * part, n), dtype) for dtype in dtypes],
        cost_estimate=pl.CostEstimate(flops=16 * part * tokens * n, bytes_accessed=16 * part * n * 4, transcendentals=0),
        compiler_params=pltpu.CompilerParams(dimension_semantics=("arbitrary",)),
        name="kept_product")(index, left, right, got)


def product_task(left, right, bits, left_axis):
    core, x, y = bits
    m = left.shape[left_axis]
    half, part = m // 2, m // 16
    chosen = lax.dynamic_slice_in_dim(left, (1 - core) * half, half, left_axis)
    to_partner = lax.dot_general(chosen, right, (((1 - left_axis,), (0,)), ((), ())), preferred_element_type=jnp.float32).astype(jnp.bfloat16)
    (from_partner,) = yield ((swap_core, to_partner),)
    send_a, send_b, keep_a, keep_b = kept_product(left, right, from_partner, bits, left_axis)
    got_a, got_b = yield ((swap_x, send_a), (swap_y, send_b))

    def twice(keep, got, which):
        return lax.dynamic_slice_in_dim(keep, which * part, part, 0) + lax.dynamic_slice_in_dim(got, which * part, part, 0).astype(jnp.float32)

    more_a, more_b = yield ((swap_y, twice(keep_a, got_a, 1 - y).astype(jnp.bfloat16)),
                            (swap_x, twice(keep_b, got_b, 1 - x).astype(jnp.bfloat16)))
    own_a = (twice(keep_a, got_a, y) + more_a.astype(jnp.float32)).astype(jnp.bfloat16)
    own_b = (twice(keep_b, got_b, x) + more_b.astype(jnp.float32)).astype(jnp.bfloat16)
    return row_major(jnp.concatenate([own_a, own_b], 0))


def scatter_task(keep, send, bits):
    _, x, y = bits
    got = yield tuple((swap_core, part) for part in send)
    own = [(part + other.astype(jnp.float32)).reshape(2, 2, *part.shape[1:]) for part, other in zip(keep, got)]

    def pick(a, axis, index):
        return lax.dynamic_index_in_dim(a, index, axis, keepdims=False)

    got = yield ((swap_x, pick(own[0], 1, 1 - x).astype(jnp.bfloat16)), (swap_y, pick(own[1], 0, 1 - y).astype(jnp.bfloat16)))
    own = [pick(own[0], 1, x) + got[0].astype(jnp.float32), pick(own[1], 0, y) + got[1].astype(jnp.float32)]
    got = yield ((swap_y, pick(own[0], 0, 1 - y).astype(jnp.bfloat16)), (swap_x, pick(own[1], 0, 1 - x).astype(jnp.bfloat16)))
    return [pick(own[0], 0, y) + got[0].astype(jnp.float32), pick(own[1], 0, x) + got[1].astype(jnp.float32)]


def vector_task(vectors):
    flat = jnp.concatenate([v.reshape(-1) for v in vectors])
    flat = jnp.pad(flat, (0, -flat.size % 1024)).reshape(-1, 1024)
    for swap in (swap_core, swap_x, swap_y):
        (got,) = yield ((swap, flat),)
        flat = flat + got
    return flat.reshape(-1)


class Exchanges:
    def __init__(self, bits):
        self.bits = bits
        self.running = []
        self.products = set()
        self.results = {}
        self.fillers = []
        self.filled = {}

    def add(self, name, task):
        self.running.append([name, task, None])

    def product(self, name, left, right, left_axis):
        self.products.add(name)
        self.add(name, product_task(left, right, self.bits, left_axis))

    def fill(self, name, compute):
        self.fillers.append((name, compute))

    def slot(self, main, fill=0):
        names = list(self.filled)
        main, arrived, filled = tie(main, [pending for _, _, pending in self.running], [self.filled[name] for name in names])
        self.filled.update(zip(names, filled))
        still, outgoing = [], []
        for (name, task, _), got in zip(self.running, arrived):
            try:
                sends = next(task) if got is None else task.send(got)
            except StopIteration as finished:
                if name in self.products:
                    outgoing.append(finished.value)
                    self.results[name] = row_major(lax.all_gather(finished.value, SEQ_AXIS))
                else:
                    self.results[name] = finished.value
                continue
            still.append([name, task, tuple(swap(value) for swap, value in sends)])
            outgoing.append([value for _, value in sends])
        due = [name for name, _ in self.fillers[:fill] if name in self.products]
        main, _, gathered = tie(main, outgoing, [self.results[name] for name in due])
        self.results.update(zip(due, gathered))
        self.running = still
        for name, compute in self.fillers[:fill]:
            self.filled[name] = compute()
        self.fillers = self.fillers[fill:]
        return main

    def place(self, name, rows, into=None, first_row=0):
        return place_blocks(self.results[name], into, rows, first_row)

    def vectors(self, name, shapes):
        flat, start, result = self.results[name], 0, []
        for v in shapes:
            result.append(flat[start:start + v.size].reshape(v.shape))
            start += v.size
        return result


def device_bits(my_rank):
    return my_rank % 2, (my_rank // 2) % 2, my_rank // 4


def layer_norm(x_f, gain, shift):
    row_mean = jnp.mean(x_f, axis=-1, keepdims=True)
    centred = x_f - row_mean
    row_var = jnp.mean(centred * centred, axis=-1, keepdims=True)
    return centred * lax.rsqrt(row_var + LN_EPS) * gain + shift


def gelu_tanh(pre_act):
    return jax.nn.gelu(pre_act, approximate=True)


def dot_tn(a, b):
    return lax.dot_general(a, b, (((0,), (0,)), ((), ())), preferred_element_type=jnp.float32)


def dot_nn(a, b):
    return lax.dot_general(a, b, (((1,), (0,)), ((), ())), preferred_element_type=jnp.float32)


def dot_nt(a, b):
    return lax.dot_general(a, b, (((1,), (1,)), ((), ())), preferred_element_type=jnp.float32)


def query_minus_key(n_keys, n_queries):
    return lax.broadcasted_iota(jnp.int32, (n_keys, n_queries), 1) - lax.broadcasted_iota(jnp.int32, (n_keys, n_queries), 0)


def score_factor(head):
    return head ** -0.5 * LOG2E


def dense_forward_kernel(rank_ref, q_ref, k_ref, v_ref, o_ref, lse_ref):
    rank = rank_ref[0]
    q = q_ref[...]
    head, block = q.shape

    def step(j, carry, diagonal=False):
        top, total, acc = carry
        scores = dot_tn(k_ref[j], q) * score_factor(head)
        if diagonal:
            scores = jnp.where(query_minus_key(block, block) >= 0, scores, MASKED)
        new_top = jnp.maximum(top, jnp.max(scores, axis=0, keepdims=True))
        shrink = jnp.exp2(top - new_top)
        probs = jnp.exp2(scores - new_top)
        total = total * shrink + jnp.sum(probs, axis=0, keepdims=True)
        acc = acc * shrink + dot_nn(v_ref[j], probs.astype(jnp.bfloat16))
        return new_top, total, acc

    start = (jnp.full((1, block), MASKED, jnp.float32), jnp.zeros((1, block), jnp.float32), jnp.zeros((head, block), jnp.float32))
    top, total, acc = step(rank, lax.fori_loop(0, rank, step, start), diagonal=True)
    o_ref[...] = (acc / total).astype(jnp.bfloat16)
    lse_ref[0] = top + jnp.log2(total)


def dense_backward_kernel(rank_ref, q_ref, k_ref, v_ref, o_ref, do_ref, lse_ref,
                          dq_ref, dk_keep_ref, dv_keep_ref, dk_send_ref, dv_send_ref):
    rank = rank_ref[0]
    core = lax.rem(rank, 2)
    q, d_out = q_ref[...], do_ref[...]
    head, block = q.shape
    scale = head ** -0.5
    delta = jnp.sum(o_ref[...].astype(jnp.float32) * d_out.astype(jnp.float32), axis=0, keepdims=True)
    lse = lse_ref[0]
    dq_ref[...] = jnp.zeros_like(dq_ref)

    def block_grads(j, diagonal):
        k, v = k_ref[j], v_ref[j]
        scores = dot_tn(k, q) * score_factor(head)
        if diagonal:
            scores = jnp.where(query_minus_key(block, block) >= 0, scores, MASKED)
        probs = jnp.exp2(scores - lse)
        d_scores = (probs * (dot_tn(v, d_out) - delta)).astype(jnp.bfloat16)
        dq_ref[...] += dot_nn(k, d_scores) * scale
        return dot_nt(q, d_scores) * scale, dot_nt(d_out, probs.astype(jnp.bfloat16))

    def fill(pair, j, dk_ref, dv_ref, diagonals):
        for diagonal in diagonals:
            @pl.when(j == rank if diagonal else j < rank)
            def _(diagonal=diagonal):
                dk, dv = block_grads(j, diagonal)
                dk_ref[pair] = dk.astype(dk_ref.dtype)
                dv_ref[pair] = dv.astype(dv_ref.dtype)

        @pl.when(j > rank)
        def _():
            dk_ref[pair] = jnp.zeros(dk_ref.shape[1:], dk_ref.dtype)
            dv_ref[pair] = jnp.zeros(dv_ref.shape[1:], dv_ref.dtype)

    def step(pair, carry):
        fill(pair, 2 * pair + core, dk_keep_ref, dv_keep_ref, (False, True))
        fill(pair, 2 * pair + 1 - core, dk_send_ref, dv_send_ref, (False,))
        return carry

    lax.fori_loop(0, 4, step, 0)


def band_mask(rank, half):
    diff = query_minus_key(2 * WINDOW, WINDOW)
    allowed = (diff < 0) & (diff >= -WINDOW)
    if half == 0:
        first_key = jnp.where(rank == 0, WINDOW, 0)
        allowed = allowed & (lax.broadcasted_iota(jnp.int32, (2 * WINDOW, WINDOW), 0) >= first_key)
    return allowed


def band_forward_kernel(rank_ref, q_ref, k_ref, v_ref, o_ref, lse_ref):
    head = q_ref.shape[0]
    for half in range(2):
        at_q, at_k = pl.ds(half * WINDOW, WINDOW), pl.ds(half * WINDOW, 2 * WINDOW)
        scores = dot_tn(k_ref[:, at_k], q_ref[:, at_q]) * score_factor(head)
        scores = jnp.where(band_mask(rank_ref[0], half), scores, MASKED)
        top = jnp.max(scores, axis=0, keepdims=True)
        probs = jnp.exp2(scores - top)
        total = jnp.sum(probs, axis=0, keepdims=True)
        out = dot_nn(v_ref[:, at_k], probs.astype(jnp.bfloat16))
        o_ref[:, at_q] = (out / total).astype(jnp.bfloat16)
        lse_ref[0, :, at_q] = top + jnp.log2(total)


def band_backward_kernel(rank_ref, q_ref, k_ref, v_ref, o_ref, do_ref, lse_ref, dq_ref, dk_ref, dv_ref):
    head = q_ref.shape[0]
    scale = head ** -0.5
    for half in range(2):
        at_q, at_k = pl.ds(half * WINDOW, WINDOW), pl.ds(half * WINDOW, 2 * WINDOW)
        q, d_out, k, v = q_ref[:, at_q], do_ref[:, at_q], k_ref[:, at_k], v_ref[:, at_k]
        delta = jnp.sum(o_ref[:, at_q].astype(jnp.float32) * d_out.astype(jnp.float32), axis=0, keepdims=True)
        scores = dot_tn(k, q) * score_factor(head)
        scores = jnp.where(band_mask(rank_ref[0], half), scores, MASKED)
        probs = jnp.exp2(scores - lse_ref[0, :, at_q])
        d_scores = (probs * (dot_tn(v, d_out) - delta)).astype(jnp.bfloat16)
        dq_ref[:, at_q] = dot_nn(k, d_scores) * scale
        for out_ref, value in ((dk_ref, dot_nt(q, d_scores) * scale), (dv_ref, dot_nt(d_out, probs.astype(jnp.bfloat16)))):
            if half == 0:
                out_ref[:, pl.ds(0, 2 * WINDOW)] = value
            else:
                out_ref[:, pl.ds(WINDOW, WINDOW)] += value[:, :WINDOW]
                out_ref[:, pl.ds(2 * WINDOW, WINDOW)] = value[:, WINDOW:]


def head_call(kernel, name, rank, heads, operands, out_shapes, flops):
    def spec(shape, offset):
        if shape[-2] == 1:
            return pl.BlockSpec((1,) + shape[1:], lambda h, rank_ref: (h + offset, 0, 0))
        if len(shape) == 2:
            return pl.BlockSpec((HEAD, shape[1]), lambda h, rank_ref: (h + offset, 0))
        return pl.BlockSpec((shape[0], HEAD, shape[2]), lambda h, rank_ref: (0, h + offset, 0))

    grid_spec = pltpu.PrefetchScalarGridSpec(
        num_scalar_prefetch=1, grid=(heads,),
        in_specs=[spec(a.shape, offset) for a, offset in operands],
        out_specs=[spec(s.shape, 0) for s in out_shapes])
    return pl.pallas_call(
        kernel, grid_spec=grid_spec, out_shape=out_shapes,
        cost_estimate=pl.CostEstimate(flops=flops, bytes_accessed=sum(a.size * 2 for a, _ in operands), transcendentals=0),
        compiler_params=pltpu.CompilerParams(dimension_semantics=("arbitrary",)), name=name)(rank, *[a for a, _ in operands])


def shape_of(*shape, dtype=jnp.float32):
    return jax.ShapeDtypeStruct(shape, dtype)


def layer_forward(x_in, layer_wts, banded, rank, n_dev):
    (n1_gain, n1_bias, qkv_w, qkv_b, out_w, out_b, n2_gain, n2_bias, up_w, up_b, down_w, down_b) = layer_wts
    x_f = x_in.astype(jnp.float32)
    hid_one = layer_norm(x_f, n1_gain.astype(jnp.float32), n1_bias.astype(jnp.float32)).astype(jnp.bfloat16)
    hidden = out_w.shape[0] * out_w.shape[1]
    qkv_w2 = qkv_w.reshape(-1, 3 * hidden)

    def project(start, count):
        rows = lax.dot_general(qkv_w2[:, start:start + count], hid_one, (((0,), (1,)), ((), ())), preferred_element_type=jnp.float32)
        return (rows + qkv_b.reshape(-1)[start:start + count, None].astype(jnp.float32)).astype(jnp.bfloat16)

    if banded:
        qkv_t = project(0, 3 * hidden)
        q_t, kv_t = qkv_t[:hidden], qkv_t[hidden:]
        block = q_t.shape[1]
        to_next = [(source, source + 1) for source in range(n_dev - 1)]
        prev_tail = lax.ppermute(kv_t[:, block - WINDOW:], SEQ_AXIS, to_next)
        context = jnp.concatenate([prev_tail, kv_t], axis=1)
        attn_t, lse = head_call(band_forward_kernel, "band_forward", rank, HEADS,
                                [(q_t, 0), (context, 0), (context, HEADS)],
                                [shape_of(hidden, block, dtype=jnp.bfloat16), shape_of(HEADS, 1, block)], 4_000_000_000)
    else:
        q_t, kv_t = project(0, hidden), project(hidden, 2 * hidden)
        context = []
        size = hidden // GROUPS
        for g in range(GROUPS):
            part = jnp.concatenate([kv_t[g * size:(g + 1) * size], kv_t[hidden + g * size:hidden + (g + 1) * size]], 0)
            part = row_major(lax.all_gather(row_major(part), SEQ_AXIS))
            context.append((part, part))
        outs = [head_call(dense_forward_kernel, "dense_forward", rank, HEADS // GROUPS,
                          [(q_t, g * (HEADS // GROUPS)), (k_all, 0), (v_all, HEADS // GROUPS)],
                          [shape_of(size, q_t.shape[1], dtype=jnp.bfloat16), shape_of(HEADS // GROUPS, 1, q_t.shape[1])], 12_000_000_000)
                for g, (k_all, v_all) in enumerate(context)]
        attn_t, lse = jnp.concatenate([o for o, _ in outs], 0), [part for _, part in outs]
    x_mid = (x_f + lax.dot_general(attn_t, out_w.reshape(hidden, -1), (((0,), (0,)), ((), ())), preferred_element_type=jnp.float32)
             + out_b.astype(jnp.float32)).astype(jnp.bfloat16)
    mid_f = x_mid.astype(jnp.float32)
    hid_two = layer_norm(mid_f, n2_gain.astype(jnp.float32), n2_bias.astype(jnp.float32)).astype(jnp.bfloat16)
    up_pre = dot_nn(hid_two, up_w) + up_b.astype(jnp.float32)
    up_act = gelu_tanh(up_pre).astype(jnp.bfloat16)

    def output():
        return (mid_f + dot_nn(up_act, down_w) + down_b.astype(jnp.float32)).astype(jnp.bfloat16)

    return output, (x_f, hid_one, q_t, context, lse, attn_t, mid_f, hid_two, up_pre, up_act)


def layer_backward(d_out, layer_wts, saved_acts, banded, rank, n_dev, comm, tag):
    n1_gain, n1_bias, qkv_w, out_w = layer_wts[0], layer_wts[1], layer_wts[2], layer_wts[4]
    n2_gain, n2_bias, up_w, down_w = layer_wts[6], layer_wts[7], layer_wts[8], layer_wts[10]
    (x_f, hid_one, q_t, context, lse, attn_t, mid_f, hid_two, up_pre, up_act) = saved_acts
    hidden, block = q_t.shape
    d_out16 = d_out.astype(jnp.bfloat16)
    comm.product(tag + "down_w", up_act, d_out16, 1)
    d_out, d_out16 = comm.slot((d_out, d_out16))
    g_down_b = jnp.sum(d_out, axis=0)
    d_act = dot_nt(d_out16, down_w)
    d_up = jax.vjp(gelu_tanh, up_pre)[1](d_act)[0]
    d_up16 = d_up.astype(jnp.bfloat16)
    g_up_b = jnp.sum(d_up, axis=0)
    comm.product(tag + "up_w", hid_two.T, d_up16, 0)
    (d_up16,) = comm.slot((d_up16,))
    d_hid_two = dot_nt(d_up16, up_w)
    norm2_pull = jax.vjp(layer_norm, mid_f, n2_gain.astype(jnp.float32), n2_bias.astype(jnp.float32))[1]
    d_mid_norm, g_n2_gain, g_n2_bias = norm2_pull(d_hid_two)
    d_mid = d_out + d_mid_norm
    d_mid16 = d_mid.astype(jnp.bfloat16)
    comm.product(tag + "out_w", attn_t, d_mid16, 0)
    d_mid, d_mid16 = comm.slot((d_mid, d_mid16))
    g_out_b = jnp.sum(d_mid, axis=0)
    d_attn_t = dot_nt(out_w.reshape(hidden, -1), d_mid16).astype(jnp.bfloat16)
    if banded:
        d_q, d_k, d_v = head_call(band_backward_kernel, "band_backward", rank, HEADS,
                                  [(q_t, 0), (context, 0), (context, HEADS), (attn_t, 0), (d_attn_t, 0), (lse, 0)],
                                  [shape_of(hidden, block), shape_of(hidden, block + WINDOW), shape_of(hidden, block + WINDOW)],
                                  10_000_000_000)
        to_prev = [(source + 1, source) for source in range(n_dev - 1)]
        tails = jnp.concatenate([d_k[:, :WINDOW], d_v[:, :WINDOW]], 0).astype(jnp.bfloat16)
        from_next = lax.ppermute(tails, SEQ_AXIS, to_prev)
        d_q, d_k, d_v, from_next = comm.slot((d_q, d_k, d_v, from_next))
        from_next = jnp.pad(from_next.astype(jnp.float32), ((0, 0), (block - WINDOW, 0)))
        d_k = d_k[:, WINDOW:] + from_next[:hidden]
        d_v = d_v[:, WINDOW:] + from_next[hidden:]
    else:
        heads, size = HEADS // GROUPS, hidden // GROUPS
        d_q, d_k, d_v = [], [], []
        for g, (k_all, v_all) in enumerate(context):
            half = [shape_of(4, size, block, dtype=dtype) for dtype in (jnp.float32, jnp.float32, jnp.bfloat16, jnp.bfloat16)]
            dq_g, dk_keep, dv_keep, dk_send, dv_send = head_call(
                dense_backward_kernel, "dense_backward", rank, heads,
                [(q_t, g * heads), (k_all, 0), (v_all, heads), (attn_t, g * heads), (d_attn_t, g * heads), (lse[g], 0)],
                [shape_of(size, block)] + half, 30_000_000_000)
            d_q.append(dq_g)
            comm.add("d_kv%d" % g, scatter_task((dk_keep, dv_keep), (dk_send, dv_send), comm.bits))
            (d_attn_t, d_q) = comm.slot((d_attn_t, d_q))
        d_q = jnp.concatenate(d_q, 0)
        comm.product(tag + "q_w", d_q.astype(jnp.bfloat16), hid_one, 0)
        for count in (3, 2, 0):
            (d_q,) = comm.slot((d_q,), fill=count)
        for g in range(GROUPS):
            dk_g, dv_g = comm.results["d_kv%d" % g]
            d_k.append(dk_g)
            d_v.append(dv_g)
        d_k, d_v = (jnp.concatenate(parts, 0) for parts in (d_k, d_v))
    d_qkv = jnp.concatenate([d_q, d_k, d_v], 0)
    g_qkv_b = jnp.sum(d_qkv, axis=1)
    d_qkv16 = d_qkv.astype(jnp.bfloat16)
    if banded:
        comm.product(tag + "qkv_w", d_qkv16, hid_one, 0)
    else:
        comm.product(tag + "kv_w", d_qkv16[hidden:], hid_one, 0)
    d_mid, d_qkv16 = comm.slot((d_mid, d_qkv16))
    d_hid_one = lax.dot_general(d_qkv16, qkv_w.reshape(-1, 3 * hidden), (((0,), (1,)), ((), ())), preferred_element_type=jnp.float32)
    norm1_pull = jax.vjp(layer_norm, x_f, n1_gain.astype(jnp.float32), n1_bias.astype(jnp.float32))[1]
    d_in_norm, g_n1_gain, g_n1_bias = norm1_pull(d_hid_one)
    small = (g_n1_gain, g_n1_bias, g_qkv_b, g_out_b, g_n2_gain, g_n2_bias, g_up_b, g_down_b)
    comm.add(tag + "small", vector_task(small))
    return d_mid + d_in_norm, small


def layer_gradients(comm, tag, small, layer_wts, placed):
    qkv_w, out_w = layer_wts[2], layer_wts[4]
    g_n1_gain, g_n1_bias, g_qkv_b, g_out_b, g_n2_gain, g_n2_bias, g_up_b, g_down_b = comm.vectors(tag + "small", small)
    g_qkv_w = placed[tag + "qkv_w"].reshape(qkv_w.shape[1:] + qkv_w.shape[:1]).transpose(3, 0, 1, 2)
    g_out_w = placed[tag + "out_w"].reshape(out_w.shape)
    g_qkv_b = g_qkv_b.reshape(qkv_w.shape[1:])
    return (g_n1_gain, g_n1_bias, g_qkv_w, g_qkv_b, g_out_w, g_out_b, g_n2_gain, g_n2_bias,
            placed[tag + "up_w"], g_up_b, placed[tag + "down_w"], g_down_b)


def solution(mesh):
    n_dev = mesh.shape[SEQ_AXIS]

    def sharded_step(act_in, grad_out, *weights):
        my_rank = lax.axis_index(SEQ_AXIS)
        bits = device_bits(my_rank)
        rank = my_rank.reshape(1).astype(jnp.int32)
        act_mid, saved_one = layer_forward(act_in[0], weights[:12], False, rank, n_dev)
        act_out, saved_two = layer_forward(act_mid(), weights[12:], True, rank, n_dev)
        comm = Exchanges(bits)
        comm.fill("y", act_out)
        width, inner = act_in.shape[2], weights[8].shape[1]
        rows = {"down_w": inner, "up_w": width, "out_w": width, "qkv_w": 3 * width}
        for name, count in rows.items():
            comm.fill("2" + name, functools.partial(comm.place, "2" + name, count))
        d_mid, small_two = layer_backward(grad_out[0].astype(jnp.float32), weights[12:], saved_two, True, rank, n_dev, comm, "2")
        d_in, small_one = layer_backward(d_mid, weights[:12], saved_one, False, rank, n_dev, comm, "1")
        for name in ("down_w", "up_w", "out_w"):
            comm.fill("1" + name, functools.partial(comm.place, "1" + name, rows[name]))
        while comm.running or comm.fillers:
            (d_in,) = comm.slot((d_in,), fill=1)
        placed = dict(comm.filled)
        placed["1qkv_w"] = comm.place("1kv_w", 3 * width, comm.place("1q_w", 3 * width), width)
        grads_one = layer_gradients(comm, "1", small_one, weights[:12], placed)
        grads_two = layer_gradients(comm, "2", small_two, weights[12:], placed)
        return (comm.filled["y"][None], d_in.astype(jnp.bfloat16)[None]) + grads_one + grads_two

    seq_spec = P(None, SEQ_AXIS, None)
    specs_in = (seq_spec, seq_spec) + (P(),) * 24
    specs_out = (seq_spec, seq_spec) + (P(),) * 24
    return jax.shard_map(sharded_step, mesh=mesh, in_specs=specs_in, out_specs=specs_out, check_vma=False)
```

```python
import functools

import jax
import jax.numpy as jnp
from jax import lax
from jax.experimental import pallas as pl
from jax.experimental.layout import Layout, with_layout_constraint
from jax.experimental.pallas import tpu as pltpu
from jax.sharding import PartitionSpec as P

SEQ_AXIS = "cp"
WINDOW = 256
LN_EPS = 1e-5
HEADS = 16
HEAD = 96
GROUPS = 2
BACKWARD_GROUPS = 4
LOG2E = 1.4426950408889634
MASKED = -1e30
CORE_PAIRS = tuple((i, i ^ 1) for i in range(8))
X_PAIRS = tuple((i, i ^ 2) for i in range(8))
Y_PAIRS = tuple((i, i ^ 4) for i in range(8))


def swap_core(a):
    return lax.ppermute(a, SEQ_AXIS, CORE_PAIRS)


def swap_x(a):
    return lax.ppermute(a, SEQ_AXIS, X_PAIRS)


def swap_y(a):
    return lax.ppermute(a, SEQ_AXIS, Y_PAIRS)


def row_major(a):
    return with_layout_constraint(a, Layout(major_to_minor=tuple(range(a.ndim))))


def place_kernel(gathered_ref, *refs):
    refs[-1][...] = gathered_ref[0].astype(jnp.float32)


def place_blocks(gathered, into, total_rows, first_rows):
    n = gathered.shape[2]
    rows = gathered.shape[1] // 2
    first = [row // rows for row in first_rows]

    def target(device, part):
        core, x, y = device % 2, (device // 2) % 2, device // 4
        return jnp.where(core == 0, first[0], first[1]) + part * 4 + jnp.where(part == 0, x * 2 + y, y * 2 + x), 0

    operands = [gathered] if into is None else [gathered, into]
    return pl.pallas_call(
        place_kernel, grid=(8, 2),
        in_specs=[pl.BlockSpec((1, rows, n), lambda device, part: (device, part, 0))] + [pl.BlockSpec(memory_space=pl.ANY)] * (len(operands) - 1),
        out_specs=pl.BlockSpec((rows, n), target),
        out_shape=jax.ShapeDtypeStruct((total_rows, n), jnp.float32),
        input_output_aliases={} if into is None else {1: 0},
        cost_estimate=pl.CostEstimate(flops=gathered.size, bytes_accessed=gathered.size * 6, transcendentals=0),
        compiler_params=pltpu.CompilerParams(dimension_semantics=("arbitrary", "arbitrary")),
        name="place_blocks")(*operands)


def tie(*values):
    return lax.optimization_barrier(values)


def kept_kernel(left_axis, index_ref, left_ref, right_ref, got_ref, *out_refs):
    value = lax.dot_general(left_ref[...], right_ref[...], (((1 - left_axis,), (0,)), ((), ())), preferred_element_type=jnp.float32)
    value = value + got_ref[...].astype(jnp.float32)
    for k, out_ref in enumerate(out_refs):
        @pl.when(pl.program_id(0) == k)
        def _(out_ref=out_ref):
            out_ref[...] = value.astype(out_ref.dtype)


def kept_product(left, right, got, bits, left_axis):
    core, x, y = bits
    tokens, n = right.shape
    part = left.shape[left_axis] // 8
    index = jnp.stack([1 - x, 2 + (1 - y), x, 2 + y])
    index = jnp.concatenate([index, index + core * 4]).astype(jnp.int32)
    if left_axis == 0:
        left_spec = pl.BlockSpec((part, tokens), lambda i, index_ref: (index_ref[4 + i], 0))
    else:
        left_spec = pl.BlockSpec((tokens, part), lambda i, index_ref: (0, index_ref[4 + i]))

    grid_spec = pltpu.PrefetchScalarGridSpec(
        num_scalar_prefetch=1, grid=(4,),
        in_specs=[left_spec, pl.BlockSpec((tokens, n), lambda i, index_ref: (0, 0)), pl.BlockSpec((part, n), lambda i, index_ref: (index_ref[i], 0))],
        out_specs=[pl.BlockSpec((part, n), lambda i, index_ref: (0, 0))] * 4)
    dtypes = (jnp.bfloat16, jnp.bfloat16, jnp.float32, jnp.float32)
    return pl.pallas_call(
        functools.partial(kept_kernel, left_axis), grid_spec=grid_spec,
        out_shape=[jax.ShapeDtypeStruct((part, n), dtype) for dtype in dtypes],
        cost_estimate=pl.CostEstimate(flops=part * tokens * n // 2, bytes_accessed=8 * part * n * 4, transcendentals=0),
        compiler_params=pltpu.CompilerParams(dimension_semantics=("arbitrary",)),
        name="kept_product")(index, left, right, got)


def product_task(left, right, bits, left_axis):
    core, x, y = bits
    m = left.shape[left_axis]
    half, part = m // 2, m // 16
    chosen = lax.dynamic_slice_in_dim(left, (1 - core) * half, half, left_axis)
    to_partner = lax.dot_general(chosen, right, (((1 - left_axis,), (0,)), ((), ())), preferred_element_type=jnp.float32).astype(jnp.bfloat16)
    (from_partner,) = yield ((swap_core, to_partner),)
    send_a, send_b, keep_a, keep_b = kept_product(left, right, from_partner, bits, left_axis)
    got_a, got_b = yield ((swap_x, send_a), (swap_y, send_b))

    def twice(keep, got, which):
        return lax.dynamic_slice_in_dim(keep, which * part, part, 0) + lax.dynamic_slice_in_dim(got, which * part, part, 0).astype(jnp.float32)

    more_a, more_b = yield ((swap_y, twice(keep_a, got_a, 1 - y).astype(jnp.bfloat16)),
                            (swap_x, twice(keep_b, got_b, 1 - x).astype(jnp.bfloat16)))
    own_a = (twice(keep_a, got_a, y) + more_a.astype(jnp.float32)).astype(jnp.bfloat16)
    own_b = (twice(keep_b, got_b, x) + more_b.astype(jnp.float32)).astype(jnp.bfloat16)
    return row_major(jnp.concatenate([own_a, own_b], 0))


def scatter_task(keep, send, bits):
    _, x, y = bits
    (got,) = yield ((swap_core, send),)
    own = (keep + got.astype(jnp.float32)).reshape(2, 2, *keep.shape[1:])
    own = [own[:, :, 0], own[:, :, 1]]

    def pick(a, axis, index):
        return lax.dynamic_index_in_dim(a, index, axis, keepdims=False)

    got = yield ((swap_x, pick(own[0], 1, 1 - x).astype(jnp.bfloat16)), (swap_y, pick(own[1], 0, 1 - y).astype(jnp.bfloat16)))
    own = [pick(own[0], 1, x) + got[0].astype(jnp.float32), pick(own[1], 0, y) + got[1].astype(jnp.float32)]
    got = yield ((swap_y, pick(own[0], 0, 1 - y).astype(jnp.bfloat16)), (swap_x, pick(own[1], 0, 1 - x).astype(jnp.bfloat16)))
    return [pick(own[0], 0, y) + got[0].astype(jnp.float32), pick(own[1], 0, x) + got[1].astype(jnp.float32)]


def moved_task(value, pairs):
    (got,) = yield ((lambda a: lax.ppermute(a, SEQ_AXIS, pairs), value),)
    return got


def vector_task(vectors):
    flat = jnp.concatenate([v.reshape(-1) for v in vectors])
    flat = jnp.pad(flat, (0, -flat.size % 1024)).reshape(-1, 1024)
    for swap in (swap_core, swap_x, swap_y):
        (got,) = yield ((swap, flat),)
        flat = flat + got
    return flat.reshape(-1)


class Exchanges:
    def __init__(self, bits):
        self.bits = bits
        self.running = []
        self.products = set()
        self.results = {}
        self.fillers = []
        self.filled = {}

    def add(self, name, task):
        self.running.append([name, task, None])

    def product(self, name, left, right, left_axis):
        self.products.add(name)
        self.add(name, product_task(left, right, self.bits, left_axis))

    def fill(self, name, compute):
        self.fillers.append((name, compute))

    def slot(self, main, fill=0):
        names = list(self.filled)
        main, arrived, filled = tie(main, [pending for _, _, pending in self.running], [self.filled[name] for name in names])
        self.filled.update(zip(names, filled))
        still, outgoing = [], []
        for (name, task, _), got in zip(self.running, arrived):
            try:
                sends = next(task) if got is None else task.send(got)
            except StopIteration as finished:
                if name in self.products:
                    outgoing.append(finished.value)
                    self.results[name] = row_major(lax.all_gather(finished.value, SEQ_AXIS))
                else:
                    self.results[name] = finished.value
                continue
            still.append([name, task, tuple(swap(value) for swap, value in sends)])
            outgoing.append([value for _, value in sends])
        due = [name for name, _ in self.fillers[:fill] if name in self.products]
        main, _, gathered = tie(main, outgoing, [self.results[name] for name in due])
        self.results.update(zip(due, gathered))
        self.running = still
        for name, compute in self.fillers[:fill]:
            self.filled[name] = compute()
        self.fillers = self.fillers[fill:]
        return main

    def place(self, name, rows, into=None, first_rows=None):
        return place_blocks(self.results[name], into, rows, first_rows or (0, rows // 2))

    def vectors(self, name, shapes):
        flat, start, result = self.results[name], 0, []
        for v in shapes:
            result.append(flat[start:start + v.size].reshape(v.shape))
            start += v.size
        return result


def device_bits(my_rank):
    return my_rank % 2, (my_rank // 2) % 2, my_rank // 4


def layer_norm(x_f, gain, shift):
    row_mean = jnp.mean(x_f, axis=-1, keepdims=True)
    centred = x_f - row_mean
    row_var = jnp.mean(centred * centred, axis=-1, keepdims=True)
    return centred * lax.rsqrt(row_var + LN_EPS) * gain + shift


def gelu_tanh(pre_act):
    return jax.nn.gelu(pre_act, approximate=True)


def dot_tn(a, b):
    return lax.dot_general(a, b, (((0,), (0,)), ((), ())), preferred_element_type=jnp.float32)


def dot_nn(a, b):
    return lax.dot_general(a, b, (((1,), (0,)), ((), ())), preferred_element_type=jnp.float32)


def dot_nt(a, b):
    return lax.dot_general(a, b, (((1,), (1,)), ((), ())), preferred_element_type=jnp.float32)


def query_minus_key(n_keys, n_queries):
    return lax.broadcasted_iota(jnp.int32, (n_keys, n_queries), 1) - lax.broadcasted_iota(jnp.int32, (n_keys, n_queries), 0)


def score_factor(head):
    return head ** -0.5 * LOG2E


def dense_forward_kernel(rank_ref, q_ref, k_ref, v_ref, o_ref, lse_ref):
    rank = rank_ref[0]
    q = q_ref[...]
    head, block = q.shape

    def step(j, carry, diagonal=False):
        top, total, acc = carry
        scores = dot_tn(k_ref[j], q) * score_factor(head)
        if diagonal:
            scores = jnp.where(query_minus_key(block, block) >= 0, scores, MASKED)
        new_top = jnp.maximum(top, jnp.max(scores, axis=0, keepdims=True))
        shrink = jnp.exp2(top - new_top)
        probs = jnp.exp2(scores - new_top)
        total = total * shrink + jnp.sum(probs, axis=0, keepdims=True)
        acc = acc * shrink + dot_nn(v_ref[j], probs.astype(jnp.bfloat16))
        return new_top, total, acc

    start = (jnp.full((1, block), MASKED, jnp.float32), jnp.zeros((1, block), jnp.float32), jnp.zeros((head, block), jnp.float32))
    top, total, acc = step(rank, lax.fori_loop(0, rank, step, start), diagonal=True)
    o_ref[...] = (acc / total).astype(jnp.bfloat16)
    lse_ref[0] = top + jnp.log2(total)


def dense_backward_kernel(rank_ref, q_ref, k_ref, v_ref, o_ref, do_ref, lse_ref,
                          dq_ref, keep_ref, send_ref):
    rank = rank_ref[0]
    core = lax.rem(rank, 2)
    q, d_out = q_ref[...], do_ref[...]
    head, block = q.shape
    scale = head ** -0.5
    delta = jnp.sum(o_ref[...].astype(jnp.float32) * d_out.astype(jnp.float32), axis=0, keepdims=True)
    lse = lse_ref[0]
    dq_ref[...] = jnp.zeros_like(dq_ref)

    def block_grads(j, diagonal):
        k, v = k_ref[j], v_ref[j]
        scores = dot_tn(k, q) * score_factor(head)
        if diagonal:
            scores = jnp.where(query_minus_key(block, block) >= 0, scores, MASKED)
        probs = jnp.exp2(scores - lse)
        d_scores = (probs * (dot_tn(v, d_out) - delta)).astype(jnp.bfloat16)
        dq_ref[...] += dot_nn(k, d_scores) * scale
        return dot_nt(q, d_scores) * scale, dot_nt(d_out, probs.astype(jnp.bfloat16))

    def fill(pair, j, out_ref, diagonals):
        for diagonal in diagonals:
            @pl.when(j == rank if diagonal else j < rank)
            def _(diagonal=diagonal):
                dk, dv = block_grads(j, diagonal)
                out_ref[pair, 0] = dk.astype(out_ref.dtype)
                out_ref[pair, 1] = dv.astype(out_ref.dtype)

        @pl.when(j > rank)
        def _():
            out_ref[pair] = jnp.zeros(out_ref.shape[1:], out_ref.dtype)

    def step(pair, carry):
        fill(pair, 2 * pair + core, keep_ref, (False, True))
        fill(pair, 2 * pair + 1 - core, send_ref, (False,))
        return carry

    lax.fori_loop(0, 4, step, 0)


def band_mask(rank, half):
    diff = query_minus_key(2 * WINDOW, WINDOW)
    allowed = (diff < 0) & (diff >= -WINDOW)
    if half == 0:
        first_key = jnp.where(rank == 0, WINDOW, 0)
        allowed = allowed & (lax.broadcasted_iota(jnp.int32, (2 * WINDOW, WINDOW), 0) >= first_key)
    return allowed


def band_forward_kernel(rank_ref, q_ref, k_ref, v_ref, o_ref, lse_ref):
    head = q_ref.shape[0]
    for half in range(2):
        at_q, at_k = pl.ds(half * WINDOW, WINDOW), pl.ds(half * WINDOW, 2 * WINDOW)
        scores = dot_tn(k_ref[:, at_k], q_ref[:, at_q]) * score_factor(head)
        scores = jnp.where(band_mask(rank_ref[0], half), scores, MASKED)
        top = jnp.max(scores, axis=0, keepdims=True)
        probs = jnp.exp2(scores - top)
        total = jnp.sum(probs, axis=0, keepdims=True)
        out = dot_nn(v_ref[:, at_k], probs.astype(jnp.bfloat16))
        o_ref[:, at_q] = (out / total).astype(jnp.bfloat16)
        lse_ref[0, :, at_q] = top + jnp.log2(total)


def band_backward_kernel(rank_ref, q_ref, k_ref, v_ref, o_ref, do_ref, lse_ref, dq_ref, dk_ref, dv_ref):
    head = q_ref.shape[0]
    scale = head ** -0.5
    for half in range(2):
        at_q, at_k = pl.ds(half * WINDOW, WINDOW), pl.ds(half * WINDOW, 2 * WINDOW)
        q, d_out, k, v = q_ref[:, at_q], do_ref[:, at_q], k_ref[:, at_k], v_ref[:, at_k]
        delta = jnp.sum(o_ref[:, at_q].astype(jnp.float32) * d_out.astype(jnp.float32), axis=0, keepdims=True)
        scores = dot_tn(k, q) * score_factor(head)
        scores = jnp.where(band_mask(rank_ref[0], half), scores, MASKED)
        probs = jnp.exp2(scores - lse_ref[0, :, at_q])
        d_scores = (probs * (dot_tn(v, d_out) - delta)).astype(jnp.bfloat16)
        dq_ref[:, at_q] = dot_nn(k, d_scores) * scale
        for out_ref, value in ((dk_ref, dot_nt(q, d_scores) * scale), (dv_ref, dot_nt(d_out, probs.astype(jnp.bfloat16)))):
            if half == 0:
                out_ref[:, pl.ds(0, 2 * WINDOW)] = value
            else:
                out_ref[:, pl.ds(WINDOW, WINDOW)] += value[:, :WINDOW]
                out_ref[:, pl.ds(2 * WINDOW, WINDOW)] = value[:, WINDOW:]


def head_call(kernel, name, rank, heads, operands, out_shapes, flops):
    def spec(shape, offset):
        if shape[-2] == 1:
            return pl.BlockSpec((1,) + shape[1:], lambda h, rank_ref: (h + offset, 0, 0))
        if len(shape) == 4:
            return pl.BlockSpec(shape[:2] + (HEAD, shape[3]), lambda h, rank_ref: (0, 0, h + offset, 0))
        if len(shape) == 2:
            return pl.BlockSpec((HEAD, shape[1]), lambda h, rank_ref: (h + offset, 0))
        return pl.BlockSpec((shape[0], HEAD, shape[2]), lambda h, rank_ref: (0, h + offset, 0))

    grid_spec = pltpu.PrefetchScalarGridSpec(
        num_scalar_prefetch=1, grid=(heads,),
        in_specs=[spec(a.shape, offset) for a, offset in operands],
        out_specs=[spec(s.shape, 0) for s in out_shapes])
    return pl.pallas_call(
        kernel, grid_spec=grid_spec, out_shape=out_shapes,
        cost_estimate=pl.CostEstimate(flops=flops, bytes_accessed=sum(a.size * 2 for a, _ in operands), transcendentals=0),
        compiler_params=pltpu.CompilerParams(dimension_semantics=("arbitrary",)), name=name)(rank, *[a for a, _ in operands])


def shape_of(*shape, dtype=jnp.float32):
    return jax.ShapeDtypeStruct(shape, dtype)


def layer_forward(x_in, layer_wts, banded, rank, n_dev):
    (n1_gain, n1_bias, qkv_w, qkv_b, out_w, out_b, n2_gain, n2_bias, up_w, up_b, down_w, down_b) = layer_wts
    x_f = x_in.astype(jnp.float32)
    hid_one = layer_norm(x_f, n1_gain.astype(jnp.float32), n1_bias.astype(jnp.float32)).astype(jnp.bfloat16)
    hidden = out_w.shape[0] * out_w.shape[1]
    qkv_w2 = qkv_w.reshape(-1, 3 * hidden)

    def project(start, count):
        rows = lax.dot_general(qkv_w2[:, start:start + count], hid_one, (((0,), (1,)), ((), ())), preferred_element_type=jnp.float32)
        return (rows + qkv_b.reshape(-1)[start:start + count, None].astype(jnp.float32)).astype(jnp.bfloat16)

    if banded:
        qkv_t = project(0, 3 * hidden)
        q_t, kv_t = qkv_t[:hidden], qkv_t[hidden:]
        block = q_t.shape[1]
        to_next = [(source, source + 1) for source in range(n_dev - 1)]
        prev_tail = lax.ppermute(kv_t[:, block - WINDOW:], SEQ_AXIS, to_next)
        context = jnp.concatenate([prev_tail, kv_t], axis=1)
        attn_t, lse = head_call(band_forward_kernel, "band_forward", rank, HEADS,
                                [(q_t, 0), (context, 0), (context, HEADS)],
                                [shape_of(hidden, block, dtype=jnp.bfloat16), shape_of(HEADS, 1, block)], 400_000_000)
    else:
        q_t, kv_t = project(0, hidden), project(hidden, 2 * hidden)
        context = []
        size = hidden // GROUPS
        for g in range(GROUPS):
            part = jnp.concatenate([kv_t[g * size:(g + 1) * size], kv_t[hidden + g * size:hidden + (g + 1) * size]], 0)
            part = row_major(lax.all_gather(row_major(part), SEQ_AXIS))
            context.append((part, part))
        outs = [head_call(dense_forward_kernel, "dense_forward", rank, HEADS // GROUPS,
                          [(q_t, g * (HEADS // GROUPS)), (k_all, 0), (v_all, HEADS // GROUPS)],
                          [shape_of(size, q_t.shape[1], dtype=jnp.bfloat16), shape_of(HEADS // GROUPS, 1, q_t.shape[1])], 1_000_000_000)
                for g, (k_all, v_all) in enumerate(context)]
        attn_t, lse = jnp.concatenate([o for o, _ in outs], 0), [part for _, part in outs]
    x_mid = (x_f + lax.dot_general(attn_t, out_w.reshape(hidden, -1), (((0,), (0,)), ((), ())), preferred_element_type=jnp.float32)
             + out_b.astype(jnp.float32)).astype(jnp.bfloat16)
    mid_f = x_mid.astype(jnp.float32)
    hid_two = layer_norm(mid_f, n2_gain.astype(jnp.float32), n2_bias.astype(jnp.float32)).astype(jnp.bfloat16)
    up_pre = dot_nn(hid_two, up_w) + up_b.astype(jnp.float32)
    up_act = gelu_tanh(up_pre).astype(jnp.bfloat16)

    def output():
        return (mid_f + dot_nn(up_act, down_w) + down_b.astype(jnp.float32)).astype(jnp.bfloat16)

    return output, (x_f, hid_one, q_t, context, lse, attn_t, mid_f, hid_two, up_pre, up_act)


def layer_backward(d_out, layer_wts, saved_acts, banded, rank, n_dev, comm, tag):
    n1_gain, n1_bias, qkv_w, out_w = layer_wts[0], layer_wts[1], layer_wts[2], layer_wts[4]
    n2_gain, n2_bias, up_w, down_w = layer_wts[6], layer_wts[7], layer_wts[8], layer_wts[10]
    (x_f, hid_one, q_t, context, lse, attn_t, mid_f, hid_two, up_pre, up_act) = saved_acts
    hidden, block = q_t.shape
    d_out16 = d_out.astype(jnp.bfloat16)
    comm.product(tag + "down_w", up_act, d_out16, 1)
    d_out, d_out16 = comm.slot((d_out, d_out16), fill=0 if banded else 1)
    g_down_b = jnp.sum(d_out, axis=0)
    d_act = dot_nt(d_out16, down_w)
    d_up = jax.vjp(gelu_tanh, up_pre)[1](d_act)[0]
    d_up16 = d_up.astype(jnp.bfloat16)
    g_up_b = jnp.sum(d_up, axis=0)
    comm.product(tag + "up_w", hid_two.T, d_up16, 0)
    (d_up16,) = comm.slot((d_up16,), fill=0 if banded else 1)
    d_hid_two = dot_nt(d_up16, up_w)
    norm2_pull = jax.vjp(layer_norm, mid_f, n2_gain.astype(jnp.float32), n2_bias.astype(jnp.float32))[1]
    d_mid_norm, g_n2_gain, g_n2_bias = norm2_pull(d_hid_two)
    d_mid = d_out + d_mid_norm
    d_mid16 = d_mid.astype(jnp.bfloat16)
    comm.product(tag + "out_w", attn_t, d_mid16, 0)
    d_mid, d_mid16 = comm.slot((d_mid, d_mid16))
    g_out_b = jnp.sum(d_mid, axis=0)
    d_attn_t = dot_nt(out_w.reshape(hidden, -1), d_mid16).astype(jnp.bfloat16)
    if banded:
        d_q, d_k, d_v = head_call(band_backward_kernel, "band_backward", rank, HEADS,
                                  [(q_t, 0), (context, 0), (context, HEADS), (attn_t, 0), (d_attn_t, 0), (lse, 0)],
                                  [shape_of(hidden, block), shape_of(hidden, block + WINDOW), shape_of(hidden, block + WINDOW)],
                                  1_000_000_000)
        to_prev = [(source + 1, source) for source in range(n_dev - 1)]
        tails = jnp.concatenate([d_k[:, :WINDOW], d_v[:, :WINDOW]], 0).astype(jnp.bfloat16)
        comm.add(tag + "tails", moved_task(tails, to_prev))
        for _ in range(2):
            d_q, d_k, d_v = comm.slot((d_q, d_k, d_v))
        from_next = jnp.pad(comm.results[tag + "tails"].astype(jnp.float32), ((0, 0), (block - WINDOW, 0)))
        d_k = d_k[:, WINDOW:] + from_next[:hidden]
        d_v = d_v[:, WINDOW:] + from_next[hidden:]
    else:
        heads, size, share = HEADS // BACKWARD_GROUPS, hidden // BACKWARD_GROUPS, BACKWARD_GROUPS // GROUPS
        d_q = []
        for g in range(BACKWARD_GROUPS):
            kv_all, first = context[g // share][0], g % share * heads
            dq_g, keep, send = head_call(
                dense_backward_kernel, "dense_backward", rank, heads,
                [(q_t, g * heads), (kv_all, first), (kv_all, HEADS // GROUPS + first), (attn_t, g * heads), (d_attn_t, g * heads),
                 (lse[g // share], first)],
                [shape_of(size, block), shape_of(4, 2, size, block), shape_of(4, 2, size, block, dtype=jnp.bfloat16)], 1_000_000_000)
            d_q.append(dq_g)
            comm.add("d_kv%d" % g, scatter_task(keep, send, comm.bits))
            (d_attn_t, d_q) = comm.slot((d_attn_t, d_q), fill=(2, 1, 0, 0)[g])
        d_q = jnp.concatenate(d_q, 0)
        comm.product(tag + "q_w", d_q.astype(jnp.bfloat16), hid_one, 0)

        def key_values(groups):
            return [jnp.concatenate([comm.results["d_kv%d" % g][which] for g in groups], 0) for which in range(2)]

        (d_q,) = comm.slot((d_q,), fill=1)
        first_kv = key_values((0, 1))
        comm.product(tag + "kv_w0", jnp.concatenate(first_kv, 0).astype(jnp.bfloat16), hid_one, 0)
        for count in (0, 0):
            (d_q,) = comm.slot((d_q,), fill=count)
        last_kv = key_values((2, 3))
        comm.product(tag + "kv_w1", jnp.concatenate(last_kv, 0).astype(jnp.bfloat16), hid_one, 0)
        d_k, d_v = (jnp.concatenate([one, two], 0) for one, two in zip(first_kv, last_kv))
    d_qkv = jnp.concatenate([d_q, d_k, d_v], 0)
    g_qkv_b = jnp.sum(d_qkv, axis=1)
    d_qkv16 = d_qkv.astype(jnp.bfloat16)
    if banded:
        comm.product(tag + "qkv_w", d_qkv16, hid_one, 0)
    d_mid, d_qkv16 = comm.slot((d_mid, d_qkv16))
    d_hid_one = lax.dot_general(d_qkv16, qkv_w.reshape(-1, 3 * hidden), (((0,), (1,)), ((), ())), preferred_element_type=jnp.float32)
    norm1_pull = jax.vjp(layer_norm, x_f, n1_gain.astype(jnp.float32), n1_bias.astype(jnp.float32))[1]
    d_in_norm, g_n1_gain, g_n1_bias = norm1_pull(d_hid_one)
    small = (g_n1_gain, g_n1_bias, g_qkv_b, g_out_b, g_n2_gain, g_n2_bias, g_up_b, g_down_b)
    comm.add(tag + "small", vector_task(small))
    return d_mid + d_in_norm, small


def layer_gradients(comm, tag, small, layer_wts, placed):
    qkv_w, out_w = layer_wts[2], layer_wts[4]
    g_n1_gain, g_n1_bias, g_qkv_b, g_out_b, g_n2_gain, g_n2_bias, g_up_b, g_down_b = comm.vectors(tag + "small", small)
    g_qkv_w = placed[tag + "qkv_w"].reshape(qkv_w.shape[1:] + qkv_w.shape[:1]).transpose(3, 0, 1, 2)
    g_out_w = placed[tag + "out_w"].reshape(out_w.shape)
    g_qkv_b = g_qkv_b.reshape(qkv_w.shape[1:])
    return (g_n1_gain, g_n1_bias, g_qkv_w, g_qkv_b, g_out_w, g_out_b, g_n2_gain, g_n2_bias,
            placed[tag + "up_w"], g_up_b, placed[tag + "down_w"], g_down_b)


def solution(mesh):
    n_dev = mesh.shape[SEQ_AXIS]

    def sharded_step(act_in, grad_out, *weights):
        my_rank = lax.axis_index(SEQ_AXIS)
        bits = device_bits(my_rank)
        rank = my_rank.reshape(1).astype(jnp.int32)
        act_mid, saved_one = layer_forward(act_in[0], weights[:12], False, rank, n_dev)
        act_out, saved_two = layer_forward(act_mid(), weights[12:], True, rank, n_dev)
        comm = Exchanges(bits)
        width, inner = act_in.shape[2], weights[8].shape[1]
        rows = {"down_w": inner, "up_w": width, "out_w": width, "qkv_w": 3 * width}
        for layer, name in (("2", "down_w"), ("2", "up_w"), ("2", "out_w"), ("", "y"), ("2", "qkv_w"), ("1", "down_w"), ("1", "up_w"), ("1", "out_w")):
            comm.fill(layer + name, functools.partial(comm.place, layer + name, rows[name]) if layer else act_out)
        d_mid, small_two = layer_backward(grad_out[0].astype(jnp.float32), weights[12:], saved_two, True, rank, n_dev, comm, "2")
        d_in, small_one = layer_backward(d_mid, weights[:12], saved_one, False, rank, n_dev, comm, "1")
        while comm.running or comm.fillers:
            (d_in,) = comm.slot((d_in,), fill=1)
        placed = dict(comm.filled)
        total = 3 * width
        merged = comm.place("1q_w", total, None, (0, width // 2))
        for piece in range(2):
            merged = comm.place("1kv_w%d" % piece, total, merged, (width + piece * (width // 2), 2 * width + piece * (width // 2)))
        placed["1qkv_w"] = merged
        grads_one = layer_gradients(comm, "1", small_one, weights[:12], placed)
        grads_two = layer_gradients(comm, "2", small_two, weights[12:], placed)
        return (comm.filled["y"][None], d_in.astype(jnp.bfloat16)[None]) + grads_one + grads_two

    seq_spec = P(None, SEQ_AXIS, None)
    specs_in = (seq_spec, seq_spec) + (P(),) * 24
    specs_out = (seq_spec, seq_spec) + (P(),) * 24
    return jax.shard_map(sharded_step, mesh=mesh, in_specs=specs_in, out_specs=specs_out, check_vma=False)
```

```python
import functools

import jax
import jax.numpy as jnp
from jax import lax
from jax.experimental import pallas as pl
from jax.experimental.layout import Layout, with_layout_constraint
from jax.experimental.pallas import tpu as pltpu
from jax.sharding import PartitionSpec as P

SEQ_AXIS = "cp"
WINDOW = 256
LN_EPS = 1e-5
HEADS = 16
HEAD = 96
GROUPS = 2
BACKWARD_GROUPS = 4
LOG2E = 1.4426950408889634
MASKED = -1e30
CORE_PAIRS = tuple((i, i ^ 1) for i in range(8))
X_PAIRS = tuple((i, i ^ 2) for i in range(8))
Y_PAIRS = tuple((i, i ^ 4) for i in range(8))


def swap_core(a):
    return lax.ppermute(a, SEQ_AXIS, CORE_PAIRS)


def swap_x(a):
    return lax.ppermute(a, SEQ_AXIS, X_PAIRS)


def swap_y(a):
    return lax.ppermute(a, SEQ_AXIS, Y_PAIRS)


def row_major(a):
    return with_layout_constraint(a, Layout(major_to_minor=tuple(range(a.ndim))))


def place_kernel(gathered_ref, *refs):
    refs[-1][...] = gathered_ref[0].astype(jnp.float32)


def place_blocks(gathered, into, total_rows, first_rows):
    n = gathered.shape[2]
    rows = gathered.shape[1] // 2
    first = [row // rows for row in first_rows]

    def target(device, part):
        core, x, y = device % 2, (device // 2) % 2, device // 4
        return jnp.where(core == 0, first[0], first[1]) + part * 4 + jnp.where(part == 0, x * 2 + y, y * 2 + x), 0

    operands = [gathered] if into is None else [gathered, into]
    return pl.pallas_call(
        place_kernel, grid=(8, 2),
        in_specs=[pl.BlockSpec((1, rows, n), lambda device, part: (device, part, 0))] + [pl.BlockSpec(memory_space=pl.ANY)] * (len(operands) - 1),
        out_specs=pl.BlockSpec((rows, n), target),
        out_shape=jax.ShapeDtypeStruct((total_rows, n), jnp.float32),
        input_output_aliases={} if into is None else {1: 0},
        cost_estimate=pl.CostEstimate(flops=gathered.size, bytes_accessed=gathered.size * 6, transcendentals=0),
        compiler_params=pltpu.CompilerParams(dimension_semantics=("arbitrary", "arbitrary")),
        name="place_blocks")(*operands)


def tie(*values):
    return lax.optimization_barrier(values)


def kept_kernel(left_axis, index_ref, left_ref, right_ref, got_ref, *out_refs):
    value = lax.dot_general(left_ref[...], right_ref[...], (((1 - left_axis,), (0,)), ((), ())), preferred_element_type=jnp.float32)
    value = value + got_ref[...].astype(jnp.float32)
    for k, out_ref in enumerate(out_refs):
        @pl.when(pl.program_id(0) == k)
        def _(out_ref=out_ref):
            out_ref[...] = value.astype(out_ref.dtype)


def kept_product(left, right, got, bits, left_axis, stays):
    core, x, y = bits
    tokens, n = right.shape
    part = left.shape[left_axis] // 8
    index = jnp.stack([x, 2 + y] if stays else [1 - x, 2 + (1 - y)])
    index = jnp.concatenate([index, index + core * 4]).astype(jnp.int32)
    if left_axis == 0:
        left_spec = pl.BlockSpec((part, tokens), lambda i, index_ref: (index_ref[2 + i], 0))
    else:
        left_spec = pl.BlockSpec((tokens, part), lambda i, index_ref: (0, index_ref[2 + i]))

    grid_spec = pltpu.PrefetchScalarGridSpec(
        num_scalar_prefetch=1, grid=(2,),
        in_specs=[left_spec, pl.BlockSpec((tokens, n), lambda i, index_ref: (0, 0)), pl.BlockSpec((part, n), lambda i, index_ref: (index_ref[i], 0))],
        out_specs=[pl.BlockSpec((part, n), lambda i, index_ref: (0, 0))] * 2)
    return pl.pallas_call(
        functools.partial(kept_kernel, left_axis), grid_spec=grid_spec,
        out_shape=[jax.ShapeDtypeStruct((part, n), jnp.float32 if stays else jnp.bfloat16)] * 2,
        cost_estimate=pl.CostEstimate(flops=part * tokens * n // 4, bytes_accessed=2 * part * n * 4, transcendentals=0),
        compiler_params=pltpu.CompilerParams(dimension_semantics=("arbitrary",)),
        name="kept_product")(index, left, right, got)


def product_task(left, right, bits, left_axis):
    core, x, y = bits
    m = left.shape[left_axis]
    half, part = m // 2, m // 16
    chosen = lax.dynamic_slice_in_dim(left, (1 - core) * half, half, left_axis)
    to_partner = lax.dot_general(chosen, right, (((1 - left_axis,), (0,)), ((), ())), preferred_element_type=jnp.float32).astype(jnp.bfloat16)
    (from_partner,) = yield ((swap_core, to_partner),)
    send_a, send_b = kept_product(left, right, from_partner, bits, left_axis, False)
    keep_a, keep_b = kept_product(left, right, from_partner, bits, left_axis, True)
    got_a, got_b, keep_a, keep_b = yield ((swap_x, send_a), (swap_y, send_b), (None, keep_a), (None, keep_b))

    def twice(keep, got, which):
        return lax.dynamic_slice_in_dim(keep, which * part, part, 0) + lax.dynamic_slice_in_dim(got, which * part, part, 0).astype(jnp.float32)

    more_a, more_b = yield ((swap_y, twice(keep_a, got_a, 1 - y).astype(jnp.bfloat16)),
                            (swap_x, twice(keep_b, got_b, 1 - x).astype(jnp.bfloat16)))
    own_a = (twice(keep_a, got_a, y) + more_a.astype(jnp.float32)).astype(jnp.bfloat16)
    own_b = (twice(keep_b, got_b, x) + more_b.astype(jnp.float32)).astype(jnp.bfloat16)
    return row_major(jnp.concatenate([own_a, own_b], 0))


def scatter_task(keep, send, bits):
    _, x, y = bits
    (got,) = yield ((swap_core, send),)
    own = (keep + got.astype(jnp.float32)).reshape(2, 2, *keep.shape[1:])
    own = [own[:, :, 0], own[:, :, 1]]

    def pick(a, axis, index):
        return lax.dynamic_index_in_dim(a, index, axis, keepdims=False)

    got = yield ((swap_x, pick(own[0], 1, 1 - x).astype(jnp.bfloat16)), (swap_y, pick(own[1], 0, 1 - y).astype(jnp.bfloat16)))
    own = [pick(own[0], 1, x) + got[0].astype(jnp.float32), pick(own[1], 0, y) + got[1].astype(jnp.float32)]
    got = yield ((swap_y, pick(own[0], 0, 1 - y).astype(jnp.bfloat16)), (swap_x, pick(own[1], 0, 1 - x).astype(jnp.bfloat16)))
    return [pick(own[0], 0, y) + got[0].astype(jnp.float32), pick(own[1], 0, x) + got[1].astype(jnp.float32)]


def moved_task(value, pairs):
    (got,) = yield ((lambda a: lax.ppermute(a, SEQ_AXIS, pairs), value),)
    return got


def vector_task(vectors):
    flat = jnp.concatenate([v.reshape(-1) for v in vectors])
    flat = jnp.pad(flat, (0, -flat.size % 1024)).reshape(-1, 1024)
    for swap in (swap_core, swap_x, swap_y):
        (got,) = yield ((swap, flat),)
        flat = flat + got
    return flat.reshape(-1)


class Exchanges:
    def __init__(self, bits):
        self.bits = bits
        self.running = []
        self.products = set()
        self.results = {}
        self.fillers = []
        self.filled = {}

    def add(self, name, task):
        self.running.append([name, task, None])

    def product(self, name, left, right, left_axis):
        self.products.add(name)
        self.add(name, product_task(left, right, self.bits, left_axis))

    def fill(self, name, compute):
        self.fillers.append((name, compute))

    def slot(self, main, fill=0):
        names = list(self.filled)
        main, arrived, filled = tie(main, [pending for _, _, pending in self.running], [self.filled[name] for name in names])
        self.filled.update(zip(names, filled))
        still, outgoing = [], []
        for (name, task, _), got in zip(self.running, arrived):
            try:
                sends = next(task) if got is None else task.send(got)
            except StopIteration as finished:
                if name in self.products:
                    outgoing.append(finished.value)
                    self.results[name] = row_major(lax.all_gather(finished.value, SEQ_AXIS))
                else:
                    self.results[name] = finished.value
                continue
            still.append([name, task, tuple(swap(value) if swap else value for swap, value in sends)])
            outgoing.append([value for swap, value in sends if swap])
        due = [name for name, _ in self.fillers[:fill] if name in self.products]
        main, _, gathered = tie(main, outgoing, [self.results[name] for name in due])
        self.results.update(zip(due, gathered))
        self.running = still
        for name, compute in self.fillers[:fill]:
            self.filled[name] = compute()
        self.fillers = self.fillers[fill:]
        return main

    def place(self, name, rows, into=None, first_rows=None):
        return place_blocks(self.results[name], into, rows, first_rows or (0, rows // 2))

    def vectors(self, name, shapes):
        flat, start, result = self.results[name], 0, []
        for v in shapes:
            result.append(flat[start:start + v.size].reshape(v.shape))
            start += v.size
        return result


def device_bits(my_rank):
    return my_rank % 2, (my_rank // 2) % 2, my_rank // 4


def layer_norm(x_f, gain, shift):
    row_mean = jnp.mean(x_f, axis=-1, keepdims=True)
    centred = x_f - row_mean
    row_var = jnp.mean(centred * centred, axis=-1, keepdims=True)
    return centred * lax.rsqrt(row_var + LN_EPS) * gain + shift


def gelu_tanh(pre_act):
    return jax.nn.gelu(pre_act, approximate=True)


def dot_tn(a, b):
    return lax.dot_general(a, b, (((0,), (0,)), ((), ())), preferred_element_type=jnp.float32)


def dot_nn(a, b):
    return lax.dot_general(a, b, (((1,), (0,)), ((), ())), preferred_element_type=jnp.float32)


def dot_nt(a, b):
    return lax.dot_general(a, b, (((1,), (1,)), ((), ())), preferred_element_type=jnp.float32)


def query_minus_key(n_keys, n_queries):
    return lax.broadcasted_iota(jnp.int32, (n_keys, n_queries), 1) - lax.broadcasted_iota(jnp.int32, (n_keys, n_queries), 0)


def score_factor(head):
    return head ** -0.5 * LOG2E


def dense_forward_kernel(rank_ref, q_ref, k_ref, v_ref, o_ref, lse_ref):
    rank = rank_ref[0]
    q = q_ref[...]
    head, block = q.shape

    def step(j, carry, diagonal=False):
        top, total, acc = carry
        scores = dot_tn(k_ref[j], q) * score_factor(head)
        if diagonal:
            scores = jnp.where(query_minus_key(block, block) >= 0, scores, MASKED)
        new_top = jnp.maximum(top, jnp.max(scores, axis=0, keepdims=True))
        shrink = jnp.exp2(top - new_top)
        probs = jnp.exp2(scores - new_top)
        total = total * shrink + jnp.sum(probs, axis=0, keepdims=True)
        acc = acc * shrink + dot_nn(v_ref[j], probs.astype(jnp.bfloat16))
        return new_top, total, acc

    start = (jnp.full((1, block), MASKED, jnp.float32), jnp.zeros((1, block), jnp.float32), jnp.zeros((head, block), jnp.float32))
    top, total, acc = step(rank, lax.fori_loop(0, rank, step, start), diagonal=True)
    o_ref[...] = (acc / total).astype(jnp.bfloat16)
    lse_ref[0] = top + jnp.log2(total)


def dense_backward_kernel(rank_ref, q_ref, k_ref, v_ref, o_ref, do_ref, lse_ref,
                          dq_ref, keep_ref, send_ref):
    rank = rank_ref[0]
    core = lax.rem(rank, 2)
    q, d_out = q_ref[...], do_ref[...]
    head, block = q.shape
    scale = head ** -0.5
    delta = jnp.sum(o_ref[...].astype(jnp.float32) * d_out.astype(jnp.float32), axis=0, keepdims=True)
    lse = lse_ref[0]
    dq_ref[...] = jnp.zeros_like(dq_ref)

    def block_grads(j, diagonal):
        k, v = k_ref[j], v_ref[j]
        scores = dot_tn(k, q) * score_factor(head)
        if diagonal:
            scores = jnp.where(query_minus_key(block, block) >= 0, scores, MASKED)
        probs = jnp.exp2(scores - lse)
        d_scores = (probs * (dot_tn(v, d_out) - delta)).astype(jnp.bfloat16)
        dq_ref[...] += dot_nn(k, d_scores) * scale
        return dot_nt(q, d_scores) * scale, dot_nt(d_out, probs.astype(jnp.bfloat16))

    def fill(pair, j, out_ref, diagonals):
        for diagonal in diagonals:
            @pl.when(j == rank if diagonal else j < rank)
            def _(diagonal=diagonal):
                dk, dv = block_grads(j, diagonal)
                out_ref[pair, 0] = dk.astype(out_ref.dtype)
                out_ref[pair, 1] = dv.astype(out_ref.dtype)

        @pl.when(j > rank)
        def _():
            out_ref[pair] = jnp.zeros(out_ref.shape[1:], out_ref.dtype)

    def step(pair, carry):
        fill(pair, 2 * pair + core, keep_ref, (False, True))
        fill(pair, 2 * pair + 1 - core, send_ref, (False,))
        return carry

    lax.fori_loop(0, 4, step, 0)


def band_mask(rank, half):
    diff = query_minus_key(2 * WINDOW, WINDOW)
    allowed = (diff < 0) & (diff >= -WINDOW)
    if half == 0:
        first_key = jnp.where(rank == 0, WINDOW, 0)
        allowed = allowed & (lax.broadcasted_iota(jnp.int32, (2 * WINDOW, WINDOW), 0) >= first_key)
    return allowed


def band_forward_kernel(rank_ref, q_ref, k_ref, v_ref, o_ref, lse_ref):
    head = q_ref.shape[0]
    for half in range(2):
        at_q, at_k = pl.ds(half * WINDOW, WINDOW), pl.ds(half * WINDOW, 2 * WINDOW)
        scores = dot_tn(k_ref[:, at_k], q_ref[:, at_q]) * score_factor(head)
        scores = jnp.where(band_mask(rank_ref[0], half), scores, MASKED)
        top = jnp.max(scores, axis=0, keepdims=True)
        probs = jnp.exp2(scores - top)
        total = jnp.sum(probs, axis=0, keepdims=True)
        out = dot_nn(v_ref[:, at_k], probs.astype(jnp.bfloat16))
        o_ref[:, at_q] = (out / total).astype(jnp.bfloat16)
        lse_ref[0, :, at_q] = top + jnp.log2(total)


def band_backward_kernel(rank_ref, q_ref, k_ref, v_ref, o_ref, do_ref, lse_ref, dq_ref, dk_ref, dv_ref):
    head = q_ref.shape[0]
    scale = head ** -0.5
    for half in range(2):
        at_q, at_k = pl.ds(half * WINDOW, WINDOW), pl.ds(half * WINDOW, 2 * WINDOW)
        q, d_out, k, v = q_ref[:, at_q], do_ref[:, at_q], k_ref[:, at_k], v_ref[:, at_k]
        delta = jnp.sum(o_ref[:, at_q].astype(jnp.float32) * d_out.astype(jnp.float32), axis=0, keepdims=True)
        scores = dot_tn(k, q) * score_factor(head)
        scores = jnp.where(band_mask(rank_ref[0], half), scores, MASKED)
        probs = jnp.exp2(scores - lse_ref[0, :, at_q])
        d_scores = (probs * (dot_tn(v, d_out) - delta)).astype(jnp.bfloat16)
        dq_ref[:, at_q] = dot_nn(k, d_scores) * scale
        for out_ref, value in ((dk_ref, dot_nt(q, d_scores) * scale), (dv_ref, dot_nt(d_out, probs.astype(jnp.bfloat16)))):
            if half == 0:
                out_ref[:, pl.ds(0, 2 * WINDOW)] = value
            else:
                out_ref[:, pl.ds(WINDOW, WINDOW)] += value[:, :WINDOW]
                out_ref[:, pl.ds(2 * WINDOW, WINDOW)] = value[:, WINDOW:]


def head_call(kernel, name, rank, heads, operands, out_shapes, flops):
    def spec(shape, offset):
        if shape[-2] == 1:
            return pl.BlockSpec((1,) + shape[1:], lambda h, rank_ref: (h + offset, 0, 0))
        if len(shape) == 4:
            return pl.BlockSpec(shape[:2] + (HEAD, shape[3]), lambda h, rank_ref: (0, 0, h + offset, 0))
        if len(shape) == 2:
            return pl.BlockSpec((HEAD, shape[1]), lambda h, rank_ref: (h + offset, 0))
        return pl.BlockSpec((shape[0], HEAD, shape[2]), lambda h, rank_ref: (0, h + offset, 0))

    grid_spec = pltpu.PrefetchScalarGridSpec(
        num_scalar_prefetch=1, grid=(heads,),
        in_specs=[spec(a.shape, offset) for a, offset in operands],
        out_specs=[spec(s.shape, 0) for s in out_shapes])
    return pl.pallas_call(
        kernel, grid_spec=grid_spec, out_shape=out_shapes,
        cost_estimate=pl.CostEstimate(flops=flops, bytes_accessed=sum(a.size * 2 for a, _ in operands), transcendentals=0),
        compiler_params=pltpu.CompilerParams(dimension_semantics=("arbitrary",)), name=name)(rank, *[a for a, _ in operands])


def shape_of(*shape, dtype=jnp.float32):
    return jax.ShapeDtypeStruct(shape, dtype)


def layer_forward(x_in, layer_wts, banded, rank, n_dev):
    (n1_gain, n1_bias, qkv_w, qkv_b, out_w, out_b, n2_gain, n2_bias, up_w, up_b, down_w, down_b) = layer_wts
    x_f = x_in.astype(jnp.float32)
    hid_one = layer_norm(x_f, n1_gain.astype(jnp.float32), n1_bias.astype(jnp.float32)).astype(jnp.bfloat16)
    hidden = out_w.shape[0] * out_w.shape[1]
    qkv_w2 = qkv_w.reshape(-1, 3 * hidden)

    def project(start, count):
        rows = lax.dot_general(qkv_w2[:, start:start + count], hid_one, (((0,), (1,)), ((), ())), preferred_element_type=jnp.float32)
        return (rows + qkv_b.reshape(-1)[start:start + count, None].astype(jnp.float32)).astype(jnp.bfloat16)

    if banded:
        qkv_t = project(0, 3 * hidden)
        q_t, kv_t = qkv_t[:hidden], qkv_t[hidden:]
        block = q_t.shape[1]
        to_next = [(source, source + 1) for source in range(n_dev - 1)]
        prev_tail = lax.ppermute(kv_t[:, block - WINDOW:], SEQ_AXIS, to_next)
        context = jnp.concatenate([prev_tail, kv_t], axis=1)
        attn_t, lse = head_call(band_forward_kernel, "band_forward", rank, HEADS,
                                [(q_t, 0), (context, 0), (context, HEADS)],
                                [shape_of(hidden, block, dtype=jnp.bfloat16), shape_of(HEADS, 1, block)], 400_000_000)
    else:
        q_t, kv_t = project(0, hidden), project(hidden, 2 * hidden)
        context = []
        size = hidden // GROUPS
        for g in range(GROUPS):
            part = jnp.concatenate([kv_t[g * size:(g + 1) * size], kv_t[hidden + g * size:hidden + (g + 1) * size]], 0)
            part = row_major(lax.all_gather(row_major(part), SEQ_AXIS))
            context.append((part, part))
        outs = [head_call(dense_forward_kernel, "dense_forward", rank, HEADS // GROUPS,
                          [(q_t, g * (HEADS // GROUPS)), (k_all, 0), (v_all, HEADS // GROUPS)],
                          [shape_of(size, q_t.shape[1], dtype=jnp.bfloat16), shape_of(HEADS // GROUPS, 1, q_t.shape[1])], 1_000_000_000)
                for g, (k_all, v_all) in enumerate(context)]
        attn_t, lse = jnp.concatenate([o for o, _ in outs], 0), [part for _, part in outs]
    x_mid = (x_f + lax.dot_general(attn_t, out_w.reshape(hidden, -1), (((0,), (0,)), ((), ())), preferred_element_type=jnp.float32)
             + out_b.astype(jnp.float32)).astype(jnp.bfloat16)
    mid_f = x_mid.astype(jnp.float32)
    hid_two = layer_norm(mid_f, n2_gain.astype(jnp.float32), n2_bias.astype(jnp.float32)).astype(jnp.bfloat16)
    up_pre = dot_nn(hid_two, up_w) + up_b.astype(jnp.float32)
    up_act = gelu_tanh(up_pre).astype(jnp.bfloat16)

    def output():
        return (mid_f + dot_nn(up_act, down_w) + down_b.astype(jnp.float32)).astype(jnp.bfloat16)

    return output, (x_f, hid_one, q_t, context, lse, attn_t, mid_f, hid_two, up_pre, up_act)


def layer_backward(d_out, layer_wts, saved_acts, banded, rank, n_dev, comm, tag):
    n1_gain, n1_bias, qkv_w, out_w = layer_wts[0], layer_wts[1], layer_wts[2], layer_wts[4]
    n2_gain, n2_bias, up_w, down_w = layer_wts[6], layer_wts[7], layer_wts[8], layer_wts[10]
    (x_f, hid_one, q_t, context, lse, attn_t, mid_f, hid_two, up_pre, up_act) = saved_acts
    hidden, block = q_t.shape
    d_out16 = d_out.astype(jnp.bfloat16)
    comm.product(tag + "down_w", up_act, d_out16, 1)
    d_out, d_out16 = comm.slot((d_out, d_out16), fill=0 if banded else 1)
    g_down_b = jnp.sum(d_out, axis=0)
    d_act = dot_nt(d_out16, down_w)
    d_up = jax.vjp(gelu_tanh, up_pre)[1](d_act)[0]
    d_up16 = d_up.astype(jnp.bfloat16)
    g_up_b = jnp.sum(d_up, axis=0)
    comm.product(tag + "up_w", hid_two.T, d_up16, 0)
    (d_up16,) = comm.slot((d_up16,), fill=0 if banded else 1)
    d_hid_two = dot_nt(d_up16, up_w)
    norm2_pull = jax.vjp(layer_norm, mid_f, n2_gain.astype(jnp.float32), n2_bias.astype(jnp.float32))[1]
    d_mid_norm, g_n2_gain, g_n2_bias = norm2_pull(d_hid_two)
    d_mid = d_out + d_mid_norm
    d_mid16 = d_mid.astype(jnp.bfloat16)
    comm.product(tag + "out_w", attn_t, d_mid16, 0)
    d_mid, d_mid16 = comm.slot((d_mid, d_mid16))
    g_out_b = jnp.sum(d_mid, axis=0)
    d_attn_t = dot_nt(out_w.reshape(hidden, -1), d_mid16).astype(jnp.bfloat16)
    if banded:
        d_q, d_k, d_v = head_call(band_backward_kernel, "band_backward", rank, HEADS,
                                  [(q_t, 0), (context, 0), (context, HEADS), (attn_t, 0), (d_attn_t, 0), (lse, 0)],
                                  [shape_of(hidden, block), shape_of(hidden, block + WINDOW), shape_of(hidden, block + WINDOW)],
                                  1_000_000_000)
        to_prev = [(source + 1, source) for source in range(n_dev - 1)]
        tails = jnp.concatenate([d_k[:, :WINDOW], d_v[:, :WINDOW]], 0).astype(jnp.bfloat16)
        comm.add(tag + "tails", moved_task(tails, to_prev))
        for _ in range(2):
            d_q, d_k, d_v = comm.slot((d_q, d_k, d_v))
        from_next = jnp.pad(comm.results[tag + "tails"].astype(jnp.float32), ((0, 0), (block - WINDOW, 0)))
        d_k = d_k[:, WINDOW:] + from_next[:hidden]
        d_v = d_v[:, WINDOW:] + from_next[hidden:]
    else:
        heads, size, share = HEADS // BACKWARD_GROUPS, hidden // BACKWARD_GROUPS, BACKWARD_GROUPS // GROUPS
        d_q = []
        for g in range(BACKWARD_GROUPS):
            kv_all, first = context[g // share][0], g % share * heads
            dq_g, keep, send = head_call(
                dense_backward_kernel, "dense_backward", rank, heads,
                [(q_t, g * heads), (kv_all, first), (kv_all, HEADS // GROUPS + first), (attn_t, g * heads), (d_attn_t, g * heads),
                 (lse[g // share], first)],
                [shape_of(size, block), shape_of(4, 2, size, block), shape_of(4, 2, size, block, dtype=jnp.bfloat16)], 1_000_000_000)
            d_q.append(dq_g)
            comm.add("d_kv%d" % g, scatter_task(keep, send, comm.bits))
            (d_attn_t, d_q) = comm.slot((d_attn_t, d_q), fill=(2, 1, 0, 1)[g])
        d_q = jnp.concatenate(d_q, 0)
        comm.product(tag + "q_w", d_q.astype(jnp.bfloat16), hid_one, 0)

        def key_values(groups):
            return [jnp.concatenate([comm.results["d_kv%d" % g][which] for g in groups], 0) for which in range(2)]

        (d_q,) = comm.slot((d_q,))
        first_kv = key_values((0, 1))
        comm.product(tag + "kv_w0", jnp.concatenate(first_kv, 0).astype(jnp.bfloat16), hid_one, 0)
        for count in (1, 0):
            (d_q,) = comm.slot((d_q,), fill=count)
        last_kv = key_values((2, 3))
        comm.product(tag + "kv_w1", jnp.concatenate(last_kv, 0).astype(jnp.bfloat16), hid_one, 0)
        d_k, d_v = (jnp.concatenate([one, two], 0) for one, two in zip(first_kv, last_kv))
    d_qkv = jnp.concatenate([d_q, d_k, d_v], 0)
    g_qkv_b = jnp.sum(d_qkv, axis=1)
    d_qkv16 = d_qkv.astype(jnp.bfloat16)
    if banded:
        comm.product(tag + "qkv_w", d_qkv16, hid_one, 0)
    d_mid, d_qkv16 = comm.slot((d_mid, d_qkv16))
    d_hid_one = lax.dot_general(d_qkv16, qkv_w.reshape(-1, 3 * hidden), (((0,), (1,)), ((), ())), preferred_element_type=jnp.float32)
    norm1_pull = jax.vjp(layer_norm, x_f, n1_gain.astype(jnp.float32), n1_bias.astype(jnp.float32))[1]
    d_in_norm, g_n1_gain, g_n1_bias = norm1_pull(d_hid_one)
    small = (g_n1_gain, g_n1_bias, g_qkv_b, g_out_b, g_n2_gain, g_n2_bias, g_up_b, g_down_b)
    return d_mid + d_in_norm, small


def layer_gradients(comm, tag, small, layer_wts, placed):
    qkv_w, out_w = layer_wts[2], layer_wts[4]
    g_n1_gain, g_n1_bias, g_qkv_b, g_out_b, g_n2_gain, g_n2_bias, g_up_b, g_down_b = small
    g_qkv_w = placed[tag + "qkv_w"].reshape(qkv_w.shape[1:] + qkv_w.shape[:1]).transpose(3, 0, 1, 2)
    g_out_w = placed[tag + "out_w"].reshape(out_w.shape)
    g_qkv_b = g_qkv_b.reshape(qkv_w.shape[1:])
    return (g_n1_gain, g_n1_bias, g_qkv_w, g_qkv_b, g_out_w, g_out_b, g_n2_gain, g_n2_bias,
            placed[tag + "up_w"], g_up_b, placed[tag + "down_w"], g_down_b)


def solution(mesh):
    n_dev = mesh.shape[SEQ_AXIS]

    def sharded_step(act_in, grad_out, *weights):
        my_rank = lax.axis_index(SEQ_AXIS)
        bits = device_bits(my_rank)
        rank = my_rank.reshape(1).astype(jnp.int32)
        act_mid, saved_one = layer_forward(act_in[0], weights[:12], False, rank, n_dev)
        act_out, saved_two = layer_forward(act_mid(), weights[12:], True, rank, n_dev)
        comm = Exchanges(bits)
        width, inner = act_in.shape[2], weights[8].shape[1]
        rows = {"down_w": inner, "up_w": width, "out_w": width, "qkv_w": 3 * width}
        for layer, name in (("2", "down_w"), ("2", "up_w"), ("2", "out_w"), ("", "y"), ("2", "qkv_w"), ("1", "down_w"), ("1", "up_w"), ("1", "out_w")):
            comm.fill(layer + name, functools.partial(comm.place, layer + name, rows[name]) if layer else act_out)
        d_mid, small_two = layer_backward(grad_out[0].astype(jnp.float32), weights[12:], saved_two, True, rank, n_dev, comm, "2")
        d_in, small_one = layer_backward(d_mid, weights[:12], saved_one, False, rank, n_dev, comm, "1")
        comm.add("small", vector_task(small_one + small_two))
        while comm.running or comm.fillers:
            (d_in,) = comm.slot((d_in,), fill=1)
        placed = dict(comm.filled)
        total = 3 * width
        merged = comm.place("1q_w", total, None, (0, width // 2))
        for piece in range(2):
            merged = comm.place("1kv_w%d" % piece, total, merged, (width + piece * (width // 2), 2 * width + piece * (width // 2)))
        placed["1qkv_w"] = merged
        small_sums = comm.vectors("small", small_one + small_two)
        grads_one = layer_gradients(comm, "1", small_sums[:8], weights[:12], placed)
        grads_two = layer_gradients(comm, "2", small_sums[8:], weights[12:], placed)
        return (comm.filled["y"][None], d_in.astype(jnp.bfloat16)[None]) + grads_one + grads_two

    seq_spec = P(None, SEQ_AXIS, None)
    specs_in = (seq_spec, seq_spec) + (P(),) * 24
    specs_out = (seq_spec, seq_spec) + (P(),) * 24
    return jax.shard_map(sharded_step, mesh=mesh, in_specs=specs_in, out_specs=specs_out, check_vma=False)
```
